32 devices in a mesh: gx: 4 (over y, x), gy: 4 (over z), layer: 2 (over core).
Axes of the slice: x: 2, y: 2, z: 4, core: 2. Of those that a mesh axis runs over, the one named last changes fastest.
Arguments:
- profiles: bfloat16 [2, 4, 65536, 256], P('layer', 'gx', 'gy'), may hold values from 0.049804688 to 2
- time_weight: bfloat16 [256], replicated, may hold values from 0 to 0.029907227
- slot_cell: int32 [2, 4, 65536], P('layer', 'gx', 'gy'), may hold values from 0 to 65535
- inst_count: int32 [2, 4, 4], P('layer', 'gx', 'gy'), may hold values from 1 to 16384, as said below
- metal: float32 [6, 512, 2048], P('layer', 'gx', 'gy'), may hold values from 0.5 to 4
- via_density: float32 [512, 2048], P('gx', 'gy'), may hold values from 0.5 to 4
- pad: float32 [512, 2048], P('gx', 'gy'), may hold values from 0.05 to 0.5
- start_drop: float32 [6, 512, 2048], P('layer', 'gx', 'gy'), may hold values from 0 to 1
Outputs:
- drop: float32 [6, 512, 2048], P('layer', 'gx', 'gy')
- residual: float32 [6, 512, 2048], P('layer', 'gx', 'gy')
The draws below stay inside these ranges and needn't reach their ends.
Inputs may be any that keep to these rules, and one draw needn't show every extreme that they name: The first inst_count slots of a device are live, the rest are padding; and one device is full in every draw. `slot_cell`: row-major cell index within the tile of 128 x 512 cells.
All inputs are finite; a program needn't handle non-finite values.
Results may differ from the reference program's by a relative error of at most 0.0018.
Values sent between devices are 32-bit elements; how exact they have to be, the bound alone decides.
A program may use at most 64 MiB of HBM per device.

```python
import math
import jax
import jax.numpy as jnp

CX = 128
CY = 512
INST_DEV = 16384
TIME = 256
ITERS = 3
GROUPS = 2
TILES_X = 4
TILES_Y = 4
NL = 6
NX = 512
NY = 2048


def draw_inst_count(key, part):
    key_factor, key_group, key_column = jax.random.split(jax.random.fold_in(key, 17), 3)
    tile_rows = jnp.arange(TILES_Y, dtype=jnp.int32)
    base_count = INST_DEV * (TILES_Y - 1 + 5 * tile_rows) // (6 * (TILES_Y - 1))
    factor = jax.random.randint(key_factor, (GROUPS, TILES_X, TILES_Y), 70, 101)
    counts = jnp.maximum(base_count[None, None, :] * factor // 100, 1)
    group_pick = jax.random.randint(key_group, (), 0, GROUPS)
    column_pick = jax.random.randint(key_column, (), 0, TILES_X)
    counts = counts.at[group_pick, column_pick, TILES_Y - 1].set(INST_DEV)
    return counts.astype(jnp.int32)


def with_ends(values, rng, low, top_value):
    longest = values.shape.index(max(values.shape))
    spots = []
    for shift in (0, 1):
        where = [jax.random.randint(jax.random.fold_in(rng, axis), (), 0, length) for axis, length in enumerate(values.shape)]
        where[longest] = (where[longest] + shift) % values.shape[longest]
        spots.append(tuple(where))
    return values.at[spots[0]].set(low).at[spots[1]].set(top_value)


def steps_of(key, shape, cuts, least, largest):
    gain, own = 1.0, jax.random.fold_in(key, 6)
    for axis_at, parts in cuts:
        draws = jnp.exp(jax.random.uniform(jax.random.fold_in(own, axis_at), (parts,), jnp.float32, least / len(cuts), largest / len(cuts)))
        gain = gain * jnp.repeat(draws, shape[axis_at] // parts).reshape([-1 if axis == axis_at else 1 for axis in range(len(shape))])
    return gain


def setup_inputs(seed: int = 0) -> dict:
    streams_of = jax.random.split(jax.random.key(seed), 9)
    return {
        "profiles": jnp.clip(jnp.exp(math.log(2.0) - 3.6927934 * jax.random.uniform(streams_of[0], (GROUPS, TILES_X, TILES_Y * INST_DEV, TIME), jnp.float32) ** steps_of(streams_of[0], (GROUPS, TILES_X, TILES_Y * INST_DEV, TIME), ((0, 2), (1, 4), (2, 4)), -0.2, 0.2)), 0.049804688, 2.0).astype(jnp.bfloat16),
        "time_weight": jnp.clip(jax.random.uniform(streams_of[1], (TIME,), jnp.float32, 0.0, 0.029907227), 0.0, 0.029907227).astype(jnp.bfloat16),
        "slot_cell": with_ends(jax.random.randint(streams_of[2], (GROUPS, TILES_X, TILES_Y * INST_DEV), 0, CX * CY), jax.random.fold_in(streams_of[2], 1), 0, (CX * CY) - 1).astype(jnp.int32),
        "inst_count": draw_inst_count(jax.random.fold_in(streams_of[8], 71), 0),
        "metal": jnp.clip(jnp.exp(math.log(4.0) - 2.0794415 * jax.random.uniform(streams_of[4], (NL, NX, NY), jnp.float32) ** steps_of(streams_of[4], (NL, NX, NY), ((0, 2), (1, 4), (2, 4)), -0.2, 0.2)), 0.5, 4.0),
        "via_density": jnp.clip(jnp.exp(math.log(4.0) - 2.0794415 * jax.random.uniform(streams_of[5], (NX, NY), jnp.float32) ** steps_of(streams_of[5], (NX, NY), ((0, 4), (1, 4)), -0.2, 0.2)), 0.5, 4.0),
        "pad": jnp.clip(jnp.exp(math.log(0.5) - 2.3025851 * jax.random.uniform(streams_of[6], (NX, NY), jnp.float32) ** steps_of(streams_of[6], (NX, NY), ((0, 4), (1, 4)), -0.2, 0.2)), 0.05, 0.5),
        "start_drop": jnp.clip(1.0 * jax.random.uniform(streams_of[7], (NL, NX, NY), jnp.float32) ** steps_of(streams_of[7], (NL, NX, NY), ((0, 2), (1, 4), (2, 4)), -0.2, 0.2), 0.0, 1.0),
    }


def harmonic(values, beside):
    return 2.0 * values * beside / (values + beside)


def links(extended, via_column):
    middle = extended[1:-1, 1:-1, 1:-1]
    east_link = harmonic(middle, extended[1:-1, 2:, 1:-1])
    west_link = harmonic(middle, extended[1:-1, :-2, 1:-1])
    north_link = harmonic(middle, extended[1:-1, 1:-1, 2:])
    south_link = harmonic(middle, extended[1:-1, 1:-1, :-2])
    upper_link = via_column * harmonic(middle, extended[2:, 1:-1, 1:-1])
    lower_link = via_column * harmonic(middle, extended[:-2, 1:-1, 1:-1])
    return (east_link, west_link, north_link, south_link, upper_link, lower_link)


def diagonal_of(conduct):
    east_link, west_link, north_link, south_link, upper_link, lower_link = conduct
    return east_link + west_link + north_link + south_link + upper_link + lower_link


def operate(field, extended, conduct, diagonal):
    east_link, west_link, north_link, south_link, upper_link, lower_link = conduct
    result = diagonal * field - east_link * extended[1:-1, 2:, 1:-1] - west_link * extended[1:-1, :-2, 1:-1]
    result = result - north_link * extended[1:-1, 1:-1, 2:] - south_link * extended[1:-1, 1:-1, :-2]
    return result - upper_link * extended[2:, 1:-1, 1:-1] - lower_link * extended[:-2, 1:-1, 1:-1]


def reference(profiles, time_weight, slot_cell, inst_count, metal, via_density, pad, start_drop):
    slot_current = jnp.dot(profiles.reshape(-1, TIME), time_weight, preferred_element_type=jnp.float32)
    slot_current = slot_current.reshape(GROUPS, TILES_X, TILES_Y, INST_DEV)
    positions = jnp.arange(INST_DEV, dtype=jnp.int32)
    slot_current = jnp.where(positions[None, None, None, :] < inst_count[..., None], slot_current, 0.0)
    cells = slot_cell.reshape(GROUPS, TILES_X, TILES_Y, INST_DEV)
    row_base = (jnp.arange(TILES_X, dtype=jnp.int32) * CX)[None, :, None, None]
    col_base = (jnp.arange(TILES_Y, dtype=jnp.int32) * CY)[None, None, :, None]
    flat_index = ((cells // CY + row_base) * NY + cells % CY + col_base).reshape(-1).astype(jnp.int32)
    current = jax.ops.segment_sum(slot_current.reshape(-1), flat_index, num_segments=NX * NY).reshape(NX, NY)
    rhs = jnp.zeros_like(metal).at[0].set(current.astype(metal.dtype))
    conduct = links(jnp.pad(metal, 1), via_density[None])
    diagonal = diagonal_of(conduct).at[-1].add(pad)

    def apply(field):
        return operate(field, jnp.pad(field, 1), conduct, diagonal)

    solution = start_drop
    residual = rhs - apply(start_drop)
    scaled = residual / diagonal
    direction = scaled
    energy = jnp.sum(residual * scaled)
    for iteration in range(ITERS):
        image = apply(direction)
        step_size = energy / jnp.sum(direction * image)
        solution = solution + step_size * direction
        residual = residual - step_size * image
        if iteration + 1 < ITERS:
            scaled = residual / diagonal
            energy_next = jnp.sum(residual * scaled)
            direction = scaled + (energy_next / energy) * direction
            energy = energy_next
    return solution, residual
```

```python
import functools

import jax
import jax.numpy as jnp
from jax import lax
from jax.experimental import pallas as pl
from jax.experimental.pallas import tpu as pltpu
from jax.sharding import PartitionSpec as P

ITERS = 3
PAD = 8
LANES = 128
WIDE = 256
BARRIER_AT = 6
MESH = pl.DeviceIdType.MESH


def harmonic(values, beside):
    return 2.0 * values * beside / (values + beside)


def div_by(values, size):
    if size & (size - 1) == 0:
        return lax.shift_right_logical(values, jnp.full_like(values, size.bit_length() - 1))
    return lax.div(values, size)


def rem_by(values, size):
    return values & (size - 1) if size & (size - 1) == 0 else lax.rem(values, size)


def cg_coefficients(moments):
    def form(left, right):
        total = None
        for a, x in enumerate(left):
            for b, y in enumerate(right):
                term = x * y * moments[a + b]
                total = term if total is None else total + term
        return total

    one = jnp.ones_like(moments[0])
    scaled, direction = [one], [one]
    moved = [jnp.zeros_like(one)] * ITERS
    energy = form(scaled, scaled)
    for iteration in range(ITERS):
        image = [
            (direction[c] if c < len(direction) else 0.0) - (direction[c - 1] if c else 0.0)
            for c in range(len(direction) + 1)
        ]
        step = energy / form(direction, image)
        for c, value in enumerate(direction):
            moved[c] = moved[c] + step * value
        scaled = [
            (scaled[c] if c < len(scaled) else 0.0) - step * image[c] for c in range(len(image))
        ]
        if iteration + 1 < ITERS:
            energy_next = form(scaled, scaled)
            momentum = energy_next / energy
            direction = [
                scaled[c] + (momentum * direction[c] if c < len(direction) else 0.0)
                for c in range(len(scaled))
            ]
            energy = energy_next
    return moved, scaled


def kernel(
    sizes, slots, profiles, weight_in, cells_in, count, metal_in, via_in, pad_in, start_in, drop, residual,
    weight, cells, metal, via, pad, start, isem, pbuf, psem, acc, cur_recv, dinv, diag, coef, field, rows_send, rows_recv, cols_pack, cols_send, cols_recv,
    plane_recv, col_halo, sums, gather, send_sem, recv_sem, gsend, grecv,
):
    ngx, ngy, nlayer = sizes
    total = ngx * ngy * nlayer
    nl, nr, nc = metal.shape
    gx, gy, layer = lax.axis_index("gx"), lax.axis_index("gy"), lax.axis_index("layer")
    me = (gx * ngy + gy) * nlayer + layer
    chunks = pbuf.shape[0]

    def coords(flat):
        return (flat // (ngy * nlayer), (flat // nlayer) % ngy, flat % nlayer)

    loads = [
        pltpu.make_async_copy(src, dst, isem.at[i])
        for i, (src, dst) in enumerate(
            ((cells_in, cells), (metal_in, metal), (start_in, start), (via_in, via), (pad_in, pad), (weight_in, weight))
        )
    ]
    chunk_loads = [pltpu.make_async_copy(profiles.at[i], pbuf.at[i], psem.at[i]) for i in range(chunks)]
    for op in loads[1:3] + loads[5:] + loads[:1] + chunk_loads + loads[3:5]:
        op.start()
    barrier = pltpu.get_barrier_semaphore()

    def other(at, offset, size):
        return at ^ offset if size & (size - 1) == 0 else lax.rem(at + offset, size)

    def peers(visit):
        if total <= 64:
            offsets = [(a, b, c) for a in range(ngx) for b in range(ngy) for c in range(nlayer)]
            for a, b, c in sorted(offsets[1:], key=lambda o: -(o[0].bit_count() + o[1] + 0.5 * o[2])):
                visit((other(gx, a, ngx), other(gy, b, ngy), other(layer, c, nlayer)))
        else:
            def one(k, carry):
                visit(coords(lax.rem(me + k, total)))
                return carry

            lax.fori_loop(1, total, one, 0)

    peers(lambda device: pl.semaphore_signal(barrier, inc=1, device_id=device, device_id_type=MESH))

    lane = lax.broadcasted_iota(jnp.int32, (nr, LANES), 1)

    def pack_columns(first_of, last_of, count_of):
        packed = jnp.zeros((nr, LANES), jnp.float32)
        for l in range(count_of):
            packed = jnp.where(lane == l, last_of(l), packed)
            packed = jnp.where(lane == 8 + l, first_of(l), packed)
        return packed

    def exchange(e):
        own = layer
        def copy(src, dst, k, device):
            return pltpu.make_async_remote_copy(
                src_ref=src, dst_ref=dst, send_sem=send_sem.at[e, k], recv_sem=recv_sem.at[e, k],
                device_id=device, device_id_type=MESH,
            )
        plane = (1 - own) * (nl - 1)
        if e == 0:
            planes = [(metal.at[plane], plane_recv.at[0]), (start.at[plane], plane_recv.at[1])]
        else:
            planes = [(field.at[e - 1, plane, pl.ds(PAD, nr)], plane_recv.at[e + 1])]
        partner = (gx, gy, 1 - layer)
        return {
            "down": (gx < ngx - 1, copy(rows_send.at[e, 0], rows_recv.at[e, 0], 0, (lax.min(gx + 1, ngx - 1), gy, layer))),
            "up": (gx > 0, copy(rows_send.at[e, 1], rows_recv.at[e, 1], 1, (lax.max(gx - 1, 0), gy, layer))),
            "right": (gy < ngy - 1, copy(cols_send.at[e, pl.ds(0, 8)], cols_recv.at[e, 0], 2, (gx, lax.min(gy + 1, ngy - 1), layer))),
            "left": (gy > 0, copy(cols_send.at[e, pl.ds(8, 8)], cols_recv.at[e, 1], 3, (gx, lax.max(gy - 1, 0), layer))),
            "planes": [copy(s, d, 4 + i, partner) for i, (s, d) in enumerate(planes)],
        }

    def begin(e):
        ops = exchange(e)
        for op in ops["planes"]:
            op.start()
        for name in ("down", "up", "right", "left"):
            there, op = ops[name]

            @pl.when(there)
            def _():
                op.start()

    def finish(e):
        ops = exchange(e)
        arrives = {"down": gx > 0, "up": gx < ngx - 1, "right": gy > 0, "left": gy < ngy - 1}
        places = {
            "down": rows_recv.at[e, 0], "up": rows_recv.at[e, 1],
            "right": cols_recv.at[e, 0], "left": cols_recv.at[e, 1],
        }
        for name in ("down", "up", "right", "left"):
            there, op = ops[name]

            @pl.when(there)
            def _():
                op.wait_send()

            @pl.when(arrives[name])
            def _():
                op.wait_recv()

            @pl.when(jnp.logical_not(arrives[name]))
            def _():
                places[name][...] = jnp.zeros(places[name].shape, jnp.float32)
        for op in ops["planes"]:
            op.wait()
        halo = jnp.concatenate(
            [cols_recv[e, 0], cols_recv[e, 1], jnp.zeros((LANES - 16, nr), jnp.float32)], axis=0
        )
        col_halo[...] = jnp.transpose(halo)

    loads[1].wait()
    loads[2].wait()
    both = (metal, start)
    for l in range(2 * nl):
        ref = both[l // nl]
        rows_send[0, 0, pl.ds(l, 1), :] = ref[l % nl, pl.ds(nr - 1, 1), :]
        rows_send[0, 1, pl.ds(l, 1), :] = ref[l % nl, pl.ds(0, 1), :]
    packed = pack_columns(
        lambda l: both[l // nl][l % nl, :, pl.ds(0, LANES)][:, 0:1],
        lambda l: both[l // nl][l % nl, :, pl.ds(nc - LANES, LANES)][:, LANES - 1 :],
        2 * nl,
    )
    cols_send[0] = jnp.transpose(packed)[0:16]
    halves = nc // WIDE
    high = nr * halves
    acc[...] = jnp.zeros_like(acc)
    ids = lax.broadcasted_iota(jnp.int32, (max(high, WIDE), LANES), 0).astype(jnp.float32).astype(jnp.bfloat16)
    for k in (0, 5):
        loads[k].wait()
    live = count[0]
    wide_weight = jnp.concatenate(
        [jnp.broadcast_to(weight[k : k + 1], (16, weight.shape[1])) for k in range(weight.shape[0])], axis=1
    )
    nt = (((1,), (1,)), ((), ()))
    for i in range(chunks):
        if i == min(BARRIER_AT, chunks - 1):
            pl.semaphore_wait(barrier, total - 1)
            begin(0)
        chunk_loads[i].wait()

        amounts = lax.dot_general(wide_weight, pbuf[i], nt, preferred_element_type=jnp.float32)[0:1]
        position = i * slots + lax.broadcasted_iota(jnp.int32, (1, slots), 1)
        amounts = jnp.where(position < live, amounts, 0.0).astype(jnp.bfloat16)
        cell = cells[i]
        column = rem_by(cell, nc)
        tall = div_by(column, WIDE) * nr + div_by(cell, nc)
        tall = tall.astype(jnp.float32).astype(jnp.bfloat16)
        short = rem_by(column, WIDE).astype(jnp.float32).astype(jnp.bfloat16)
        left, right = [], []
        zero, one = jnp.zeros((), jnp.bfloat16), jnp.ones((), jnp.bfloat16)
        for g in range(slots // LANES):
            part = slice(g * LANES, (g + 1) * LANES)
            left.append(jnp.where(ids[:high] == tall[:, part], jnp.broadcast_to(amounts[:, part], (high, LANES)), zero))
            right.append(jnp.where(ids[:WIDE] == short[:, part], one, zero))
        acc[...] += lax.dot_general(
            jnp.concatenate(left, axis=1), jnp.concatenate(right, axis=1), nt,
            preferred_element_type=jnp.float32,
        )

    def current_copy():
        return pltpu.make_async_remote_copy(
            src_ref=acc, dst_ref=cur_recv, send_sem=send_sem.at[0, 6], recv_sem=recv_sem.at[0, 6],
            device_id=(gx, gy, 1 - layer), device_id_type=MESH,
        )

    current_copy().start()

    loads[3].wait()
    loads[4].wait()
    finish(0)
    lane_all = lax.broadcasted_iota(jnp.int32, (nr, nc), 1)
    row_all = lax.broadcasted_iota(jnp.int32, (nr, nc), 0)

    def beside(value, above, below, before, after):
        north_of = jnp.where(lane_all == nc - 1, after, pltpu.roll(value, nc - 1, 1))
        south_of = jnp.where(lane_all == 0, before, pltpu.roll(value, 1, 1))
        east_of = jnp.where(row_all == nr - 1, below, pltpu.roll(value, nr - 1, 0))
        west_of = jnp.where(row_all == 0, above, pltpu.roll(value, 1, 0))
        return east_of, west_of, north_of, south_of

    first = layer == 0
    for l in range(nl):
        value = metal[l]
        around = beside(
            value, rows_recv[0, 0, pl.ds(l, 1), :], rows_recv[0, 1, pl.ds(l, 1), :],
            col_halo[:, l : l + 1], col_halo[:, 8 + l : 9 + l],
        )
        links = [harmonic(value, other) for other in around]
        upper = metal[l + 1] if l + 1 < nl else jnp.where(first, plane_recv[0], 0.0)
        lower = metal[l - 1] if l else jnp.where(first, 0.0, plane_recv[0])
        links += [via[...] * harmonic(value, other) for other in (upper, lower)]
        whole = links[0] + links[1] + links[2] + links[3] + links[4] + links[5]
        if l + 1 == nl:
            whole = whole + jnp.where(first, 0.0, pad[...])
        diag[l] = whole
        inverse = 1.0 / whole
        dinv[l] = inverse
        for k in range(6):
            coef[k, l] = links[k] * inverse

    def inside(l, value, upper, lower):
        around = beside(value, 0.0, 0.0, 0.0, 0.0)
        out = coef[0, l] * around[0] + coef[1, l] * around[1] + coef[2, l] * around[2] + coef[3, l] * around[3]
        if upper is not None:
            out = out + coef[4, l] * upper
        if lower is not None:
            out = out + coef[5, l] * lower
        return out

    edge = (1 - layer) * (nl - 1)
    lane_west = lane == 0
    lane_east = lane == LANES - 1

    def across(f, shift, e, plane, weigh):
        odd = jnp.zeros((1, LANES), jnp.float32)

        def narrow(tile):
            wide = jnp.sum(tile, axis=0, keepdims=True)
            return functools.reduce(jnp.add, [wide[:, k : k + LANES] for k in range(0, wide.shape[1], LANES)])

        def add(l, rows, columns, first_row, term):
            odd = None
            field[f, l, pl.ds(PAD + first_row, rows), columns] += term
            if weigh is not None:
                heavy = diag[l, pl.ds(first_row, rows), columns] * field[weigh, l, pl.ds(PAD + first_row, rows), columns]
                odd = narrow(heavy * term)
            return odd

        parts = []
        everywhere = pl.ds(0, nc)
        for l in range(nl):
            parts.append(add(l, 1, everywhere, 0, coef[1, l, pl.ds(0, 1), :] * rows_recv[e, 0, pl.ds(shift + l, 1), :]))
            parts.append(add(l, 1, everywhere, nr - 1, coef[0, l, pl.ds(nr - 1, 1), :] * rows_recv[e, 1, pl.ds(shift + l, 1), :]))
            k = shift + l
            west, east = pl.ds(0, LANES), pl.ds(nc - LANES, LANES)
            parts.append(add(l, nr, west, 0, jnp.where(lane_west, coef[3, l, :, west] * col_halo[:, k : k + 1], 0.0)))
            parts.append(add(l, nr, east, 0, jnp.where(lane_east, coef[2, l, :, east] * col_halo[:, 8 + k : 9 + k], 0.0)))
        parts.append(add(edge, nr, everywhere, 0, coef[4 + layer, edge] * plane_recv[plane]))
        if weigh is not None:
            odd = functools.reduce(jnp.add, parts)
        return odd

    def send_field(e):
        f = e - 1
        for l in range(nl):
            rows_send[e, 0, pl.ds(l, 1), :] = field[f, l, pl.ds(PAD + nr - 1, 1), :]
            rows_send[e, 1, pl.ds(l, 1), :] = field[f, l, pl.ds(PAD, 1), :]
        packed = pack_columns(
            lambda l: field[f, l, pl.ds(PAD, nr), pl.ds(0, LANES)][:, 0:1],
            lambda l: field[f, l, pl.ds(PAD, nr), pl.ds(nc - LANES, LANES)][:, LANES - 1 :],
            nl,
        )
        cols_send[e] = jnp.transpose(packed)[0:16]
        begin(e)

    for l in range(nl):
        value = start[l]
        moved = inside(l, value, start[l + 1] if l + 1 < nl else None, start[l - 1] if l else None)
        field[0, l, pl.ds(PAD, nr), :] = moved - value
    across(0, nl, 0, 1, None)
    current_copy().wait()
    gathered = acc[...] + cur_recv[...]
    current = jnp.concatenate([gathered[h * nr : (h + 1) * nr] for h in range(halves)], axis=1)
    field[0, 0, pl.ds(PAD, nr), :] += jnp.where(first, dinv[0] * current, 0.0)

    tiles = []
    for e in range(1, ITERS + 1):
        f = e - 1
        send_field(e)
        even, odd = None, None
        for l in range(nl):
            value = field[f, l, pl.ds(PAD, nr), :]
            upper = field[f, l + 1, pl.ds(PAD, nr), :] if l + 1 < nl else None
            lower = field[f, l - 1, pl.ds(PAD, nr), :] if l else None
            moved = inside(l, value, upper, lower)
            field[e, l, pl.ds(PAD, nr), :] = moved
            heavy = diag[l] * value
            a = jnp.sum(heavy * value, axis=0, keepdims=True)
            b = jnp.sum(heavy * moved, axis=0, keepdims=True)
            even = a if even is None else even + a
            odd = b if odd is None else odd + b
        finish(e)
        more = across(e, 0, e, e + 1, f)
        tiles += [even, jnp.concatenate([odd[:, :LANES] + more, odd[:, LANES:]], axis=1)]

    row = lax.broadcasted_iota(jnp.int32, (1, LANES), 1)
    packed = jnp.zeros((1, LANES), jnp.float32)
    for j, tile in enumerate(tiles):
        packed = jnp.where(row == j, jnp.sum(tile, axis=1, keepdims=True), packed)
    sums[...] = packed
    gather[me] = packed

    peers(
        lambda device: pltpu.make_async_remote_copy(
            src_ref=sums, dst_ref=gather.at[me], send_sem=gsend, recv_sem=grecv,
            device_id=device, device_id_type=MESH,
        ).start()
    )
    most = gather.at[pl.ds(0, total - 1)]
    pltpu.make_async_copy(most, most, grecv).wait()
    pltpu.make_async_copy(most, most, gsend).wait()
    summed = jnp.sum(gather[...], axis=0)
    moments = [jnp.sum(jnp.where(row == j, summed, 0.0), axis=1, keepdims=True) for j in range(2 * ITERS)]
    moved, scaled = cg_coefficients(moments)
    for l in range(nl):
        parts = [field[c, l, pl.ds(PAD, nr), :] for c in range(ITERS + 1)]
        out = start[l]
        for c in range(ITERS):
            out = out + moved[c] * parts[c]
        drop[l] = out
        rest = scaled[0] * parts[0]
        for c in range(1, ITERS + 1):
            rest = rest + scaled[c] * parts[c]
        residual[l] = diag[l] * rest


def per_device(sizes, profiles, time_weight, slot_cell, inst_count, metal, via_density, pad, start_drop):
    nl, nr, nc = metal.shape
    inst, times = profiles.shape[-2:]
    slots = min(1024, inst)
    chunks = inst // slots
    total = sizes[0] * sizes[1] * sizes[2]
    vmem = pl.BlockSpec(memory_space=pltpu.VMEM)
    hbm = pl.BlockSpec(memory_space=pltpu.HBM)
    stay = functools.partial(pltpu.with_memory_space_constraint, memory_space=pltpu.HBM)
    high = nr * (nc // WIDE)
    f32 = jnp.float32
    out = jax.ShapeDtypeStruct((nl, nr, nc), f32)
    exchanges = ITERS + 1
    return pl.pallas_call(
        functools.partial(kernel, sizes, slots),
        out_shape=(out, out),
        in_specs=[
            hbm, hbm, hbm, vmem,
            hbm, hbm, hbm, hbm,
        ],
        out_specs=(vmem, vmem),
        scratch_shapes=[
            pltpu.VMEM((times // LANES, LANES), jnp.bfloat16),
            pltpu.VMEM((chunks, 1, slots), jnp.int32),
            pltpu.VMEM((nl, nr, nc), f32),
            pltpu.VMEM((nr, nc), f32),
            pltpu.VMEM((nr, nc), f32),
            pltpu.VMEM((nl, nr, nc), f32),
            pltpu.SemaphoreType.DMA((6,)),
            pltpu.VMEM((chunks, slots, times), jnp.bfloat16),
            pltpu.SemaphoreType.DMA((chunks,)),
            pltpu.VMEM((high, WIDE), f32),
            pltpu.VMEM((high, WIDE), f32),
            pltpu.VMEM((nl, nr, nc), f32),
            pltpu.VMEM((nl, nr, nc), f32),
            pltpu.VMEM((6, nl, nr, nc), f32),
            pltpu.VMEM((exchanges, nl, nr + 2 * PAD, nc), f32),
            pltpu.VMEM((exchanges, 2, 8, nc), f32),
            pltpu.VMEM((exchanges, 2, 8, nc), f32),
            pltpu.VMEM((nr, LANES), f32),
            pltpu.VMEM((exchanges, 16, nr), f32),
            pltpu.VMEM((exchanges, 2, 8, nr), f32),
            pltpu.VMEM((exchanges + 1, nr, nc), f32),
            pltpu.VMEM((nr, LANES), f32),
            pltpu.VMEM((1, LANES), f32),
            pltpu.VMEM((total, 1, LANES), f32),
            pltpu.SemaphoreType.DMA((exchanges, 7)),
            pltpu.SemaphoreType.DMA((exchanges, 7)),
            pltpu.SemaphoreType.DMA,
            pltpu.SemaphoreType.DMA,
        ],
        compiler_params=pltpu.CompilerParams(
            collective_id=0, has_side_effects=True, vmem_limit_bytes=40 * 1024 * 1024
        ),
    )(
        stay(profiles.reshape(chunks, slots, times)), stay(time_weight.reshape(times // LANES, LANES)),
        stay(slot_cell.reshape(chunks, 1, slots)), inst_count,
        stay(metal), stay(via_density), stay(pad), stay(start_drop),
    )


def solution(mesh):
    sizes = tuple(mesh.shape[axis] for axis in ("gx", "gy", "layer"))
    in_specs = (
        P("layer", "gx", "gy", None),
        P(),
        P("layer", "gx", "gy"),
        P("layer", "gx", "gy"),
        P("layer", "gx", "gy"),
        P("gx", "gy"),
        P("gx", "gy"),
        P("layer", "gx", "gy"),
    )
    out_specs = (P("layer", "gx", "gy"), P("layer", "gx", "gy"))
    return jax.shard_map(
        functools.partial(per_device, sizes), mesh=mesh, in_specs=in_specs, out_specs=out_specs, check_vma=False
    )
```

```python
import functools

import jax
import jax.numpy as jnp
from jax import lax
from jax.experimental import pallas as pl
from jax.experimental.pallas import tpu as pltpu
from jax.sharding import PartitionSpec as P

ITERS = 3
LANES = 128
SUB = 8
WIDE = 256
TINY = 5e-31
BARRIER_AT = 6
MESH = pl.DeviceIdType.MESH


def div_by(values, size):
    if size & (size - 1) == 0:
        return lax.shift_right_logical(values, jnp.full_like(values, size.bit_length() - 1))
    return lax.div(values, size)


def rem_by(values, size):
    return values & (size - 1) if size & (size - 1) == 0 else lax.rem(values, size)


def cg_coefficients(moments):
    def form(left, right):
        total = None
        for a, x in enumerate(left):
            for b, y in enumerate(right):
                term = x * y * moments[a + b]
                total = term if total is None else total + term
        return total

    one = jnp.ones_like(moments[0])
    scaled, direction = [one], [one]
    moved = [jnp.zeros_like(one)] * ITERS
    energy = form(scaled, scaled)
    for iteration in range(ITERS):
        image = [
            (direction[c] if c < len(direction) else 0.0) - (direction[c - 1] if c else 0.0)
            for c in range(len(direction) + 1)
        ]
        step = energy / form(direction, image)
        for c, value in enumerate(direction):
            moved[c] = moved[c] + step * value
        scaled = [
            (scaled[c] if c < len(scaled) else 0.0) - step * image[c] for c in range(len(image))
        ]
        if iteration + 1 < ITERS:
            energy_next = form(scaled, scaled)
            momentum = energy_next / energy
            direction = [
                scaled[c] + (momentum * direction[c] if c < len(direction) else 0.0)
                for c in range(len(scaled))
            ]
            energy = energy_next
    return moved, scaled


def kernel(
    sizes, slots, profiles, weight_in, cells_in, count, metal_in, via_in, pad_in, start_in, drop, residual,
    weight, cells, pbuf, psem, isem,
    raw, edge, inner, row_src, col_src, row_pack, col_pack, row_recv, col_recv, corner_recv,
    acc, strips, cur_recv, cur_row, cur_col, cur_corner, col_turn, cur,
    rows_link, cols_link, up_link, dinv, field, grad, away, away_dinv, away_start,
    sums, gather, send_sem, recv_sem, part_send, part_recv, back_send, back_recv, gsend, grecv,
):
    ngx, ngy, nlayer = sizes
    total = ngx * ngy * nlayer
    nl, nr, nc = metal_in.shape
    nz = nlayer * nl
    half = nr // nlayer
    ext = half + SUB
    high = ext // SUB
    flat = nc // LANES
    tiles = flat + 1
    halves = nc // WIDE
    gx, gy, layer = lax.axis_index("gx"), lax.axis_index("gy"), lax.axis_index("layer")
    me = (gx * ngy + gy) * nlayer + layer
    chunks = pbuf.shape[0]
    first = layer == 0
    mine = layer * nl
    theirs = (1 - layer) * nl
    own_row = layer * half
    other_row = (1 - layer) * half
    own_inner = half - SUB * layer
    other_inner = half - SUB * (1 - layer)

    def coords(number):
        return (number // (ngy * nlayer), (number // nlayer) % ngy, number % nlayer)

    loads = []

    def load(src, dst):
        op = pltpu.make_async_copy(src, dst, isem.at[len(loads)])
        loads.append(op)
        return op

    def edges(ref, at):
        cut = ref.at[:, pl.ds(0, SUB)], ref.at[:, pl.ds(nr - SUB, SUB)]
        side = ref.at[:, :, pl.ds(0, LANES)], ref.at[:, :, pl.ds(nc - LANES, LANES)]
        return [load(cut[d], row_src.at[d, pl.ds(at, nl)]) for d in (0, 1)] + [
            load(side[d], col_src.at[d, pl.ds(at, nl)]) for d in (0, 1)
        ]

    def flat_edges(ref, at):
        cut = ref.at[pl.ds(0, SUB)], ref.at[pl.ds(nr - SUB, SUB)]
        side = ref.at[:, pl.ds(0, LANES)], ref.at[:, pl.ds(nc - LANES, LANES)]
        return [load(cut[d], row_src.at[d, at]) for d in (0, 1)] + [load(side[d], col_src.at[d, at]) for d in (0, 1)]

    edge_loads = edges(metal_in, 0) + edges(start_in, nl) + flat_edges(via_in, 2 * nl) + flat_edges(pad_in, 2 * nl + 1)
    slot_loads = [load(weight_in, weight), load(cells_in, cells)]
    own_loads = []
    for k, ref in enumerate((metal_in, start_in)):
        own_loads.append(load(ref.at[:, pl.ds(own_row, half)], raw.at[pl.ds(k * nz + mine, nl), pl.ds(0, half)]))
        own_loads.append(load(ref.at[:, pl.ds(own_inner, SUB)], inner.at[pl.ds(k * nz + mine, nl)]))
    for k, ref in enumerate((via_in, pad_in)):
        own_loads.append(load(ref.at[pl.ds(own_row, half)], raw.at[2 * nz + k, pl.ds(0, half)]))
        own_loads.append(load(ref.at[pl.ds(own_inner, SUB)], inner.at[2 * nz + k]))
    own_loads.append(load(start_in.at[:, pl.ds(other_row, half)], away_start))
    chunk_loads = [pltpu.make_async_copy(profiles.at[i], pbuf.at[i], psem.at[i]) for i in range(chunks)]
    for op in edge_loads + slot_loads + chunk_loads + own_loads:
        op.start()

    barrier = pltpu.get_barrier_semaphore()

    def other(at, offset, size):
        return at ^ offset if size & (size - 1) == 0 else lax.rem(at + offset, size)

    def peers(visit):
        if total <= 64:
            offsets = [(a, b, c) for a in range(ngx) for b in range(ngy) for c in range(nlayer)]
            for a, b, c in sorted(offsets[1:], key=lambda o: -(o[0].bit_count() + o[1] + 0.5 * o[2])):
                visit((other(gx, a, ngx), other(gy, b, ngy), other(layer, c, nlayer)))
        else:
            def one(k, carry):
                visit(coords(lax.rem(me + k, total)))
                return carry

            lax.fori_loop(1, total, one, 0)

    peers(lambda device: pl.semaphore_signal(barrier, inc=1, device_id=device, device_id_type=MESH))

    above, below, before, after = gx > 0, gx < ngx - 1, gy > 0, gy < ngy - 1
    gx_up, gx_down = lax.max(gx - 1, 0), lax.min(gx + 1, ngx - 1)
    gy_left, gy_right = lax.max(gy - 1, 0), lax.min(gy + 1, ngy - 1)
    outside = jnp.logical_or(jnp.logical_and(first, above), jnp.logical_and(jnp.logical_not(first), below))
    RIGHT, LEFT = 0, 1

    def exchange(stage, row_of, col_of, corner_of, row_to, col_to, corner_to):
        both = jnp.logical_and
        plan = [
            (above, (gx_up, gy, 1), row_of(0), row_to.at[layer], layer),
            (below, (gx_down, gy, 0), row_of(1), row_to.at[layer], layer),
        ]
        for there, at, side, edge_at in ((before, gy_left, RIGHT, 0), (after, gy_right, LEFT, 1)):
            for part in range(nlayer):
                plan.append((there, (gx, at, part), col_of(edge_at, part), col_to.at[side, layer], 2 + 2 * side + layer))
            plan.append((both(above, there), (gx_up, at, 1), corner_of(0, edge_at), corner_to.at[side, layer], 6 + 2 * side + layer))
            plan.append((both(below, there), (gx_down, at, 0), corner_of(1, edge_at), corner_to.at[side, layer], 6 + 2 * side + layer))
        sends = [
            (
                there,
                pltpu.make_async_remote_copy(
                    src_ref=src, dst_ref=dst, send_sem=send_sem.at[stage, k], recv_sem=recv_sem.at[stage, r],
                    device_id=device, device_id_type=MESH,
                ),
            )
            for k, (there, device, src, dst, r) in enumerate(plan)
        ]
        arrivals = [(outside, row_to, 0)]
        for there, side in ((after, RIGHT), (before, LEFT)):
            arrivals.append((there, col_to.at[side], 2 + 2 * side))
            arrivals.append((both(outside, there), corner_to.at[side], 6 + 2 * side))
        return sends, arrivals

    def begin(sends):
        for there, op in sends:
            @pl.when(there)
            def _():
                op.start()

    def sent(sends):
        for there, op in sends:
            @pl.when(there)
            def _():
                op.wait_send()

    def receive(stage, arrivals, blank):
        for there, place, at in arrivals:
            @pl.when(there)
            def _():
                for k in range(nlayer):
                    pltpu.make_async_copy(place.at[k], place.at[k], recv_sem.at[stage, at + k]).wait()

            @pl.when(jnp.logical_not(there))
            def _():
                place[...] = jnp.full(place.shape, blank, jnp.float32)

    partner = (gx, gy, 1 - layer)

    def to_partner(src, dst, send, recv):
        return pltpu.make_async_remote_copy(
            src_ref=src, dst_ref=dst, send_sem=send, recv_sem=recv, device_id=partner, device_id_type=MESH
        )

    window = [pl.ds(k * (half - SUB), ext) for k in range(nlayer)]
    halo_sends, halo_arrivals = exchange(
        0,
        lambda d: row_pack.at[d],
        lambda d, part: col_pack.at[window[part]],
        lambda r, d: col_pack.at[pl.ds((nr - SUB) * r, SUB)],
        row_recv, col_recv, corner_recv,
    )
    plane_sends = []
    for k, ref in enumerate((metal_in, start_in)):
        at = pl.ds(k * nz + mine, nl)
        for src, dst in (
            (ref.at[:, pl.ds(other_row, half)], raw.at[at, pl.ds(0, half)]),
            (ref.at[:, pl.ds(other_inner, SUB)], inner.at[at]),
        ):
            n = len(plane_sends)
            plane_sends.append(to_partner(src, dst, part_send.at[n], part_recv.at[n]))

    for op in edge_loads:
        op.wait()
    sub = lax.broadcasted_iota(jnp.int32, (SUB, nc), 0)
    pairs = [(l, nl + l) for l in range(nl)] + [(2 * nl, 2 * nl + 1)]
    for k, (a, b) in enumerate(pairs):
        low = pltpu.roll(row_src[0, b], SUB // 2, 0)
        row_pack[0, k] = jnp.where(sub < SUB // 2, row_src[0, a], low)
        low = pltpu.roll(row_src[1, b], SUB // 2, 0)
        row_pack[1, k] = jnp.where(sub < SUB // 2, low, row_src[1, a])
    lane = lax.broadcasted_iota(jnp.int32, (nr, LANES), 1)
    kinds = 2 * nl + 2
    owner = ((lane + 4) >> 3) & (LANES // 8 - 1)
    packed = jnp.ones((nr, LANES), jnp.float32)
    for q in range(kinds):
        pair = jnp.where(lane < LANES // 2, col_src[0, q], col_src[1, q])
        if q:
            pair = pltpu.roll(pair, 8 * q, 1)
        packed = jnp.where(owner == q, pair, packed)
    col_pack[...] = packed

    tall_size = nr * halves
    acc[...] = jnp.zeros_like(acc)
    ids = lax.broadcasted_iota(jnp.int32, (max(tall_size, WIDE), LANES), 0).astype(jnp.float32).astype(jnp.bfloat16)
    for op in slot_loads:
        op.wait()
    live = count[0]
    wide_weight = jnp.concatenate(
        [jnp.broadcast_to(weight[k : k + 1], (16, weight.shape[1])) for k in range(weight.shape[0])], axis=1
    )
    nt = (((1,), (1,)), ((), ()))
    for i in range(chunks):
        if i == min(BARRIER_AT, chunks - 1):
            pl.semaphore_wait(barrier, total - 1)
            begin(halo_sends)
            for op in plane_sends:
                op.start()
        chunk_loads[i].wait()
        amounts = lax.dot_general(wide_weight, pbuf[i], nt, preferred_element_type=jnp.float32)[0:1]
        position = i * slots + lax.broadcasted_iota(jnp.int32, (1, slots), 1)
        amounts = jnp.where(position < live, amounts, 0.0).astype(jnp.bfloat16)
        cell = cells[i]
        column = rem_by(cell, nc)
        tall = div_by(column, WIDE) * nr + div_by(cell, nc)
        tall = tall.astype(jnp.float32).astype(jnp.bfloat16)
        short = rem_by(column, WIDE).astype(jnp.float32).astype(jnp.bfloat16)
        left, right = [], []
        zero, one = jnp.zeros((), jnp.bfloat16), jnp.ones((), jnp.bfloat16)
        for g in range(slots // LANES):
            part = slice(g * LANES, (g + 1) * LANES)
            left.append(jnp.where(ids[:tall_size] == tall[:, part], jnp.broadcast_to(amounts[:, part], (tall_size, LANES)), zero))
            right.append(jnp.where(ids[:WIDE] == short[:, part], one, zero))
        acc[...] += lax.dot_general(
            jnp.concatenate(left, axis=1), jnp.concatenate(right, axis=1), nt,
            preferred_element_type=jnp.float32,
        ).reshape(acc.shape)

    strips[0] = jnp.transpose(acc[0, :, pl.ds(0, LANES)])[0:SUB]
    strips[1] = jnp.transpose(acc[halves - 1, :, pl.ds(WIDE - LANES, LANES)])[LANES - SUB :]
    corner_tiles = ((0, pl.ds(0, LANES)), (halves - 1, pl.ds(WIDE - LANES, LANES)))
    cur_sends, cur_arrivals = exchange(
        1,
        lambda d: acc.at[:, pl.ds((nr - SUB) * d, SUB)],
        lambda d, part: strips.at[d],
        lambda r, d: acc.at[corner_tiles[d][0], pl.ds((nr - SUB) * r, SUB), corner_tiles[d][1]],
        cur_row, cur_col, cur_corner,
    )
    n = len(plane_sends)
    cur_op = to_partner(
        acc.at[:, pl.ds((1 - layer) * (half - SUB), ext)], cur_recv, part_send.at[n], part_recv.at[n]
    )
    begin(cur_sends)
    cur_op.start()

    for op in own_loads:
        op.wait()
    for op in plane_sends:
        op.wait()
    receive(0, halo_arrivals, TINY)
    inward = (sub < SUB // 2) == first
    for k in range(nlayer):
        for l in range(nl):
            got = row_recv[k, l]
            for q, value in ((k * nl + l, got), (nz + k * nl + l, pltpu.roll(got, SUB // 2, 0))):
                raw[q, pl.ds(half, SUB)] = jnp.where(inward, inner[q], value)
    got = row_recv[0, nl]
    for q, value in ((2 * nz, got), (2 * nz + 1, pltpu.roll(got, SUB // 2, 0))):
        raw[q, pl.ds(half, SUB)] = jnp.where(inward, inner[q], value)
    lane_half = lane[:half]
    lane_sub = lane[:SUB]
    inward_tile = inward[:, :LANES]
    lane_ext = lax.broadcasted_iota(jnp.int32, (ext, LANES), 1)
    rim = jnp.logical_or(lane_ext < 4, lane_ext >= LANES - 4)
    body_at = pl.ds(pl.multiple_of(SUB * layer, SUB), half)
    inner_at = pl.ds(pl.multiple_of(half * (1 - layer), SUB), SUB)
    for k in range(nlayer):
        def side_of(tall, cut, corner):
            return jnp.where((cut & 7) < 4, tall[0], tall[1])

        main = jnp.where((lane_half & 7) < 4, col_recv[RIGHT, k, body_at], col_recv[LEFT, k, body_at])
        near = jnp.where((lane_sub & 7) < 4, col_recv[RIGHT, k, inner_at], col_recv[LEFT, k, inner_at])
        far = jnp.where((lane_sub & 7) < 4, corner_recv[RIGHT, k], corner_recv[LEFT, k])
        mixed = jnp.concatenate([main, jnp.where(inward_tile, near, far)], axis=0)
        spots = [(q, k * nl + q) for q in range(nl)] + [(nl + q, nz + k * nl + q) for q in range(nl)]
        if k == 0:
            spots += [(2 * nl, 2 * nz), (2 * nl + 1, 2 * nz + 1)]
        for q, plane in spots:
            turned = pltpu.roll(mixed, LANES - 8 * q, 1) if q else mixed
            edge[plane] = jnp.where(rim, turned, 1.0)

    shape = (tiles, high, SUB, LANES)
    sub_at = lax.broadcasted_iota(jnp.int32, shape, 2)
    lane_at = lax.broadcasted_iota(jnp.int32, shape, 3)
    last_sub, first_sub = sub_at == SUB - 1, sub_at == 0
    last_lane, first_lane = lane_at == LANES - 1, lane_at == 0

    def plane_of(q):
        value = raw[q]
        parts = [value[:, t * LANES : (t + 1) * LANES] for t in range(flat)] + [edge[q]]
        return jnp.stack([part.reshape(high, SUB, LANES) for part in parts])

    def keep(ref, at, value):
        ref[at] = value.reshape(tiles, ext, LANES)

    def held(ref, at):
        return ref[at].reshape(shape)

    def row_up(x):
        y = pltpu.roll(x.reshape(tiles * high, SUB, LANES), SUB - 1, 1).reshape(shape)
        return jnp.where(last_sub, jnp.concatenate([y[:, 1:], y[:, :1]], axis=1), y)

    def row_down(x):
        y = pltpu.roll(x.reshape(tiles * high, SUB, LANES), 1, 1).reshape(shape)
        return jnp.where(first_sub, jnp.concatenate([y[:, -1:], y[:, :-1]], axis=1), y)

    def lane_up(x):
        y = pltpu.roll(x.reshape(tiles * ext, LANES), LANES - 1, 1).reshape(shape)
        return jnp.where(last_lane, jnp.concatenate([y[1:], y[:1]], axis=0), y)

    def lane_down(x):
        y = pltpu.roll(x.reshape(tiles * ext, LANES), 1, 1).reshape(shape)
        return jnp.where(first_lane, jnp.concatenate([y[-1:], y[:-1]], axis=0), y)

    def pull(z, value, upper, lower):
        rows, cols = held(rows_link, z), held(cols_link, z)
        out = rows * row_up(value) + row_down(rows * value) + cols * lane_up(value) + lane_down(cols * value)
        if upper is not None:
            out = out + held(up_link, z) * upper
        if lower is not None:
            out = out + held(up_link, z - 1) * lower
        return out

    moments = [None] * (2 * ITERS)

    def measure(j, left, right):
        own = (left * right)[:flat, : half // SUB]
        value = jnp.sum(own.reshape(flat * (half // SUB), SUB, LANES), axis=0)
        moments[j] = value if moments[j] is None else moments[j] + value

    via = plane_of(2 * nz)
    resist = 0.5 / plane_of(0)
    for z in range(nz):
        keep(rows_link, z, 1.0 / (resist + row_up(resist)))
        keep(cols_link, z, 1.0 / (resist + lane_up(resist)))
        if z + 1 < nz:
            upper = 0.5 / plane_of(z + 1)
            keep(up_link, z, via / (resist + upper))
            resist = upper
    for z in range(nz):
        rows, cols = held(rows_link, z), held(cols_link, z)
        whole = rows + row_down(rows) + cols + lane_down(cols)
        if z + 1 < nz:
            whole = whole + held(up_link, z)
        if z:
            whole = whole + held(up_link, z - 1)
        if z + 1 == nz:
            whole = whole + plane_of(2 * nz + 1)
        inverse = 1.0 / whole
        keep(dinv, z, inverse)
        value = plane_of(nz + z)
        image = pull(z, value, plane_of(nz + z + 1) if z + 1 < nz else None, plane_of(nz + z - 1) if z else None)
        image = image - whole * value
        keep(grad.at[0], z, image)
        if z:
            scaled = inverse * image
            keep(field.at[0], z, scaled)
            measure(0, scaled, image)

    back = [
        to_partner(src.at[pl.ds(theirs, nl), pl.ds(0, flat), pl.ds(0, half)], dst, back_send.at[k], back_recv.at[k])
        for k, (src, dst) in enumerate([(grad.at[c], away.at[c]) for c in range(ITERS + 1)] + [(dinv, away_dinv)])
    ]
    back[ITERS + 1].start()

    def advance(c, z):
        source = field.at[c - 1]
        value = held(source, z)
        image = pull(z, value, held(source, z + 1) if z + 1 < nz else None, held(source, z - 1) if z else None)
        keep(grad.at[c], z, image)
        measure(2 * c - 1, value, image)
        if c < ITERS:
            scaled = held(dinv, z) * image
            keep(field.at[c], z, scaled)
            measure(2 * c, scaled, image)

    for c in range(1, ITERS + 1):
        for z in range(c + 1, nz):
            advance(c, z)

    cur_op.wait()
    receive(1, cur_arrivals, 0.0)
    whole_row = pl.ds(pl.multiple_of(own_row, SUB), half)
    inner_row = pl.ds(pl.multiple_of(own_inner, SUB), SUB)
    turned = jnp.concatenate(
        [
            cur_col[RIGHT, 0] + cur_col[RIGHT, 1],
            jnp.zeros((LANES - 2 * SUB, nr), jnp.float32),
            cur_col[LEFT, 0] + cur_col[LEFT, 1],
        ],
        axis=0,
    )
    col_turn[...] = jnp.transpose(turned)
    for t in range(tiles):
        if t < flat:
            h, at = t // (WIDE // LANES), pl.ds(t % (WIDE // LANES) * LANES, LANES)
            main = acc[h, whole_row, at] + cur_recv[h, body_at, at]
            near = acc[h, inner_row, at] + cur_recv[h, inner_at, at]
            far = cur_row[0, h, :, at] + cur_row[1, h, :, at]
        else:
            main = col_turn[whole_row]
            near = col_turn[inner_row]
            far = jnp.where(
                lane_sub < LANES // 2, cur_corner[RIGHT, 0] + cur_corner[RIGHT, 1], cur_corner[LEFT, 0] + cur_corner[LEFT, 1]
            )
        cur[t, pl.ds(0, half)] = main
        cur[t, pl.ds(half, SUB)] = jnp.where(inward_tile, near, far)
    image = held(grad.at[0], 0) + cur[...].reshape(shape)
    keep(grad.at[0], 0, image)
    scaled = held(dinv, 0) * image
    keep(field.at[0], 0, scaled)
    measure(0, scaled, image)
    back[0].start()
    for c in range(1, ITERS + 1):
        for z in range(min(c + 1, nz)):
            advance(c, z)
        back[c].start()

    row = lax.broadcasted_iota(jnp.int32, (1, LANES), 1)
    packed = jnp.zeros((1, LANES), jnp.float32)
    for j, tile in enumerate(moments):
        one_row = jnp.sum(tile, axis=0, keepdims=True)
        packed = jnp.where(row == j, jnp.sum(one_row, axis=1, keepdims=True), packed)
    sums[...] = packed
    gather[me] = packed
    peers(
        lambda device: pltpu.make_async_remote_copy(
            src_ref=sums, dst_ref=gather.at[me], send_sem=gsend, recv_sem=grecv,
            device_id=device, device_id_type=MESH,
        ).start()
    )
    for op in back:
        op.wait()
    sent(halo_sends)
    sent(cur_sends)
    most = gather.at[pl.ds(0, total - 1)]
    pltpu.make_async_copy(most, most, grecv).wait()
    pltpu.make_async_copy(most, most, gsend).wait()
    summed = jnp.sum(gather[...], axis=0)
    totals = [jnp.sum(jnp.where(row == j, summed, 0.0), axis=1, keepdims=True) for j in range(2 * ITERS)]
    moved, scaled = cg_coefficients(totals)
    own_out = pl.ds(pl.multiple_of(own_row, SUB), half)
    other_out = pl.ds(pl.multiple_of(other_row, SUB), half)
    for l in range(nl):
        for t in range(flat):
            at = pl.ds(t * LANES, LANES)
            own = pl.ds(0, half)
            for place, parts, inverse, start in (
                (own_out, [grad[c, mine + l, t, own] for c in range(ITERS + 1)], dinv[mine + l, t, own], raw[nz + mine + l, own, at]),
                (other_out, [away[c, l, t] for c in range(ITERS + 1)], away_dinv[l, t], away_start[l, :, at]),
            ):
                step = moved[0] * parts[0]
                for c in range(1, ITERS):
                    step = step + moved[c] * parts[c]
                drop[l, place, at] = start + inverse * step
                rest = scaled[0] * parts[0]
                for c in range(1, ITERS + 1):
                    rest = rest + scaled[c] * parts[c]
                residual[l, place, at] = rest


def per_device(sizes, profiles, time_weight, slot_cell, inst_count, metal, via_density, pad, start_drop):
    nl, nr, nc = metal.shape
    inst, times = profiles.shape[-2:]
    slots = min(1024, inst)
    chunks = inst // slots
    total = sizes[0] * sizes[1] * sizes[2]
    nlayer = sizes[2]
    nz, half = nl * nlayer, nr // nlayer
    ext, tiles, halves = half + SUB, nc // LANES + 1, nc // WIDE
    kinds, pairs, count = 2 * nl + 2, nl + 1, ITERS + 1
    vmem = pl.BlockSpec(memory_space=pltpu.VMEM)
    hbm = pl.BlockSpec(memory_space=pltpu.HBM)
    stay = functools.partial(pltpu.with_memory_space_constraint, memory_space=pltpu.HBM)
    out = jax.ShapeDtypeStruct((nl, nr, nc), jnp.float32)

    def room(*shape):
        return pltpu.VMEM(shape, jnp.float32)

    DMA = pltpu.SemaphoreType.DMA
    return pl.pallas_call(
        functools.partial(kernel, sizes, slots),
        out_shape=(out, out),
        in_specs=[hbm, hbm, hbm, vmem, hbm, hbm, hbm, hbm],
        out_specs=(vmem, vmem),
        scratch_shapes=[
            pltpu.VMEM((times // LANES, LANES), jnp.bfloat16),
            pltpu.VMEM((chunks, 1, slots), jnp.int32),
            pltpu.VMEM((chunks, slots, times), jnp.bfloat16),
            DMA((chunks,)),
            DMA((27,)),
            room(2 * nz + 2, ext, nc),
            room(2 * nz + 2, ext, LANES),
            room(2 * nz + 2, SUB, nc),
            room(2, kinds, SUB, nc),
            room(2, kinds, nr, LANES),
            room(2, pairs, SUB, nc),
            room(nr, LANES),
            room(nlayer, pairs, SUB, nc),
            room(2, nlayer, ext, LANES),
            room(2, nlayer, SUB, LANES),
            room(halves, nr, WIDE),
            room(2, SUB, nr),
            room(halves, ext, WIDE),
            room(nlayer, halves, SUB, WIDE),
            room(2, nlayer, SUB, nr),
            room(2, nlayer, SUB, LANES),
            room(nr, LANES),
            room(tiles, ext, LANES),
            room(nz, tiles, ext, LANES),
            room(nz, tiles, ext, LANES),
            room(nz - 1, tiles, ext, LANES),
            room(nz, tiles, ext, LANES),
            room(ITERS, nz, tiles, ext, LANES),
            room(count, nz, tiles, ext, LANES),
            room(count, nl, tiles - 1, half, LANES),
            room(nl, tiles - 1, half, LANES),
            room(nl, half, nc),
            room(1, LANES),
            room(total, 1, LANES),
            DMA((2, 10)),
            DMA((2, 10)),
            DMA((5,)),
            DMA((5,)),
            DMA((count + 1,)),
            DMA((count + 1,)),
            DMA,
            DMA,
        ],
        compiler_params=pltpu.CompilerParams(
            collective_id=0, has_side_effects=True, vmem_limit_bytes=48 * 1024 * 1024
        ),
    )(
        stay(profiles.reshape(chunks, slots, times)), stay(time_weight.reshape(times // LANES, LANES)),
        stay(slot_cell.reshape(chunks, 1, slots)), inst_count,
        stay(metal), stay(via_density), stay(pad), stay(start_drop),
    )


def solution(mesh):
    sizes = tuple(mesh.shape[axis] for axis in ("gx", "gy", "layer"))
    in_specs = (
        P("layer", "gx", "gy", None),
        P(),
        P("layer", "gx", "gy"),
        P("layer", "gx", "gy"),
        P("layer", "gx", "gy"),
        P("gx", "gy"),
        P("gx", "gy"),
        P("layer", "gx", "gy"),
    )
    out_specs = (P("layer", "gx", "gy"), P("layer", "gx", "gy"))
    return jax.shard_map(
        functools.partial(per_device, sizes), mesh=mesh, in_specs=in_specs, out_specs=out_specs, check_vma=False
    )
```

```python
import functools

import jax
import jax.numpy as jnp
from jax import lax
from jax.experimental import pallas as pl
from jax.experimental.pallas import tpu as pltpu
from jax.sharding import PartitionSpec as P

ITERS = 3
LANES = 128
SUB = 8
WIDE = 256
TINY = 5e-31
SEND_AT = 1
PARTS = 2
MESH = pl.DeviceIdType.MESH


def div_by(values, size):
    if size & (size - 1) == 0:
        return lax.shift_right_logical(values, jnp.full_like(values, size.bit_length() - 1))
    return lax.div(values, size)


def rem_by(values, size):
    return values & (size - 1) if size & (size - 1) == 0 else lax.rem(values, size)


def cg_coefficients(moments):
    def form(left, right):
        total = None
        for a, x in enumerate(left):
            for b, y in enumerate(right):
                term = x * y * moments[a + b]
                total = term if total is None else total + term
        return total

    one = jnp.ones_like(moments[0])
    scaled, direction = [one], [one]
    moved = [jnp.zeros_like(one)] * ITERS
    energy = form(scaled, scaled)
    for iteration in range(ITERS):
        image = [
            (direction[c] if c < len(direction) else 0.0) - (direction[c - 1] if c else 0.0)
            for c in range(len(direction) + 1)
        ]
        step = energy / form(direction, image)
        for c, value in enumerate(direction):
            moved[c] = moved[c] + step * value
        scaled = [
            (scaled[c] if c < len(scaled) else 0.0) - step * image[c] for c in range(len(image))
        ]
        if iteration + 1 < ITERS:
            energy_next = form(scaled, scaled)
            momentum = energy_next / energy
            direction = [
                scaled[c] + (momentum * direction[c] if c < len(direction) else 0.0)
                for c in range(len(scaled))
            ]
            energy = energy_next
    return moved, scaled


def kernel(
    sizes, slots, profiles, weight_in, cells_in, count, metal_in, via_in, pad_in, start_in, drop, residual,
    weight, cells, pbuf, psem, isem,
    raw, inner, row_src, col_src, row_pack, col_pack, row_recv, col_recv, corner_recv,
    acc_parts, acc, strips, cur_recv, cur_row, cur_col, cur_corner, col_turn, cur,
    began, rows_link, cols_link, up_link, dinv, field, grad, away, away_dinv, away_start,
    sums, gather, send_sem, recv_sem, part_send, part_recv, back_send, back_recv, gsend, grecv, ready,
):
    ngx, ngy, nlayer = sizes
    total = ngx * ngy * nlayer
    nl, nr, nc = metal_in.shape
    nz = nlayer * nl
    half = nr // nlayer
    ext = half + SUB
    high = ext // SUB
    flat = nc // LANES
    tiles = flat + 1
    halves = nc // WIDE
    gx, gy, layer = lax.axis_index("gx"), lax.axis_index("gy"), lax.axis_index("layer")
    me = (gx * ngy + gy) * nlayer + layer
    chunks = pbuf.shape[0]
    first = layer == 0
    mine = layer * nl
    theirs = (1 - layer) * nl
    own_row = layer * half
    other_row = (1 - layer) * half
    own_inner = half - SUB * layer
    other_inner = half - SUB * (1 - layer)

    def coords(number):
        return (number // (ngy * nlayer), (number // nlayer) % ngy, number % nlayer)

    loads = []

    def load(src, dst):
        op = pltpu.make_async_copy(src, dst, isem.at[len(loads)])
        loads.append(op)
        return op

    def edges(ref, at):
        cut = ref.at[:, pl.ds(0, SUB)], ref.at[:, pl.ds(nr - SUB, SUB)]
        side = ref.at[:, :, pl.ds(0, LANES)], ref.at[:, :, pl.ds(nc - LANES, LANES)]
        return [load(cut[d], row_src.at[d, pl.ds(at, nl)]) for d in (0, 1)] + [
            load(side[d], col_src.at[d, pl.ds(at, nl)]) for d in (0, 1)
        ]

    def flat_edges(ref, at):
        cut = ref.at[pl.ds(0, SUB)], ref.at[pl.ds(nr - SUB, SUB)]
        side = ref.at[:, pl.ds(0, LANES)], ref.at[:, pl.ds(nc - LANES, LANES)]
        return [load(cut[d], row_src.at[d, at]) for d in (0, 1)] + [load(side[d], col_src.at[d, at]) for d in (0, 1)]

    edge_loads = edges(metal_in, 0) + edges(start_in, nl) + flat_edges(via_in, 2 * nl) + flat_edges(pad_in, 2 * nl + 1)
    slot_loads = [load(weight_in, weight), load(cells_in, cells)]
    own_loads = []
    lanes_of = [pl.ds(t * LANES, LANES) for t in range(flat)]
    for k, ref in enumerate((metal_in, start_in)):
        for t, at in enumerate(lanes_of):
            own_loads.append(load(ref.at[:, pl.ds(own_row, half), at], raw.at[pl.ds(k * nz + mine, nl), t, pl.ds(0, half)]))
        own_loads.append(load(ref.at[:, pl.ds(own_inner, SUB)], inner.at[pl.ds(k * nz + mine, nl)]))
    for k, ref in enumerate((via_in, pad_in)):
        for t, at in enumerate(lanes_of):
            own_loads.append(load(ref.at[pl.ds(own_row, half), at], raw.at[2 * nz + k, t, pl.ds(0, half)]))
        own_loads.append(load(ref.at[pl.ds(own_inner, SUB)], inner.at[2 * nz + k]))
    for t, at in enumerate(lanes_of):
        own_loads.append(load(start_in.at[:, pl.ds(other_row, half), at], away_start.at[:, t, pl.ds(0, half)]))
    chunk_loads = [pltpu.make_async_copy(profiles.at[i], pbuf.at[i], psem.at[i]) for i in range(chunks)]
    for op in slot_loads + chunk_loads[:2] + edge_loads + chunk_loads[2:] + own_loads:
        op.start()

    barrier = pltpu.get_barrier_semaphore()

    def other(at, offset, size):
        return at ^ offset if size & (size - 1) == 0 else lax.rem(at + offset, size)

    def peers(visit):
        if total <= 64:
            offsets = [(a, b, c) for a in range(ngx) for b in range(ngy) for c in range(nlayer)]
            for a, b, c in sorted(offsets[1:], key=lambda o: -(o[0].bit_count() + o[1] + 0.5 * o[2])):
                visit((other(gx, a, ngx), other(gy, b, ngy), other(layer, c, nlayer)))
        else:
            def one(k, carry):
                visit(coords(lax.rem(me + k, total)))
                return carry

            lax.fori_loop(1, total, one, 0)

    def within(at, step, size):
        return jnp.logical_and(at + step >= 0, at + step < size)

    def spread(semaphore, reach, both_layers):
        for a in (-reach, 0, reach):
            for b in (-reach, 0, reach):
                for c in range(nlayer if both_layers else 1):
                    if (a, b, c) == (0, 0, 0) or abs(a) >= ngx or abs(b) >= ngy:
                        continue

                    @pl.when(jnp.logical_and(within(gx, a, ngx), within(gy, b, ngy)))
                    def _():
                        device = (lax.clamp(0, gx + a, ngx - 1), lax.clamp(0, gy + b, ngy - 1), other(layer, c, nlayer))
                        pl.semaphore_signal(semaphore, inc=1, device_id=device, device_id_type=MESH)

    def gathered(semaphore, reach, both_layers):
        def count(at, size):
            return 1 + (at >= reach).astype(jnp.int32) + (at + reach < size).astype(jnp.int32)

        spots = count(gx, ngx) * count(gy, ngy)
        pl.semaphore_wait(semaphore, spots * (nlayer if both_layers else 1) - 1)

    spread(barrier, 1, True)
    reaches = [1]
    while 2 * reaches[-1] < max(ngx, ngy) - 1:
        reaches.append(2 * reaches[-1])

    above, below, before, after = gx > 0, gx < ngx - 1, gy > 0, gy < ngy - 1
    gx_up, gx_down = lax.max(gx - 1, 0), lax.min(gx + 1, ngx - 1)
    gy_left, gy_right = lax.max(gy - 1, 0), lax.min(gy + 1, ngy - 1)
    outside = jnp.logical_or(jnp.logical_and(first, above), jnp.logical_and(jnp.logical_not(first), below))
    RIGHT, LEFT = 0, 1

    def exchange(stage, row_of, col_of, corner_of, row_to, col_to, corner_to):
        both = jnp.logical_and
        plan = [
            (above, (gx_up, gy, 1), row_of(0), row_to.at[layer], layer),
            (below, (gx_down, gy, 0), row_of(1), row_to.at[layer], layer),
        ]
        for there, at, side, edge_at in ((before, gy_left, RIGHT, 0), (after, gy_right, LEFT, 1)):
            for part in range(nlayer):
                plan.append((there, (gx, at, part), col_of(edge_at, part), col_to.at[side, layer], 2 + 2 * side + layer))
            plan.append((both(above, there), (gx_up, at, 1), corner_of(0, edge_at), corner_to.at[side, layer], 6 + 2 * side + layer))
            plan.append((both(below, there), (gx_down, at, 0), corner_of(1, edge_at), corner_to.at[side, layer], 6 + 2 * side + layer))
        sends = [
            (
                there,
                pltpu.make_async_remote_copy(
                    src_ref=src, dst_ref=dst, send_sem=send_sem.at[stage, k], recv_sem=recv_sem.at[stage, r],
                    device_id=device, device_id_type=MESH,
                ),
            )
            for k, (there, device, src, dst, r) in enumerate(plan)
        ]
        arrivals = [(outside, row_to, 0)]
        for there, side in ((after, RIGHT), (before, LEFT)):
            arrivals.append((there, col_to.at[side], 2 + 2 * side))
            arrivals.append((both(outside, there), corner_to.at[side], 6 + 2 * side))
        return sends, arrivals

    def begin(sends):
        for there, op in sends:
            @pl.when(there)
            def _():
                op.start()

    def sent(sends):
        for there, op in sends:
            @pl.when(there)
            def _():
                op.wait_send()

    def receive(stage, arrivals, blank):
        for there, place, at in arrivals:
            @pl.when(there)
            def _():
                for k in range(nlayer):
                    pltpu.make_async_copy(place.at[k], place.at[k], recv_sem.at[stage, at + k]).wait()

            @pl.when(jnp.logical_not(there))
            def _():
                place[...] = jnp.full(place.shape, blank, jnp.float32)

    partner = (gx, gy, 1 - layer)

    def to_partner(src, dst, send, recv):
        return pltpu.make_async_remote_copy(
            src_ref=src, dst_ref=dst, send_sem=send, recv_sem=recv, device_id=partner, device_id_type=MESH
        )

    window = [pl.ds(k * (half - SUB), ext) for k in range(nlayer)]
    halo_sends, halo_arrivals = exchange(
        0,
        lambda d: row_pack.at[d],
        lambda d, part: col_pack.at[window[part]],
        lambda r, d: col_pack.at[pl.ds((nr - SUB) * r, SUB)],
        row_recv, col_recv, corner_recv,
    )
    plane_sends = []
    for k, ref in enumerate((metal_in, start_in)):
        at = pl.ds(k * nz + mine, nl)
        for src, dst in [
            (ref.at[:, pl.ds(other_row, half), lanes_of[t]], raw.at[at, t, pl.ds(0, half)]) for t in range(flat)
        ] + [(ref.at[:, pl.ds(other_inner, SUB)], inner.at[at])]:
            n = len(plane_sends)
            plane_sends.append(to_partner(src, dst, part_send.at[n], part_recv.at[n]))

    sub = lax.broadcasted_iota(jnp.int32, (SUB, nc), 0)
    lane = lax.broadcasted_iota(jnp.int32, (nr, LANES), 1)
    kinds = 2 * nl + 2

    def pack_edges():
        for op in edge_loads:
            op.wait()
        pairs = [(l, nl + l) for l in range(nl)] + [(2 * nl, 2 * nl + 1)]
        for k, (a, b) in enumerate(pairs):
            low = pltpu.roll(row_src[0, b], SUB // 2, 0)
            row_pack[0, k] = jnp.where(sub < SUB // 2, row_src[0, a], low)
            low = pltpu.roll(row_src[1, b], SUB // 2, 0)
            row_pack[1, k] = jnp.where(sub < SUB // 2, low, row_src[1, a])
        owner = ((lane + 4) >> 3) & (LANES // 8 - 1)
        packed = jnp.ones((nr, LANES), jnp.float32)
        for q in range(kinds):
            pair = jnp.where(lane < LANES // 2, col_src[0, q], col_src[1, q])
            if q:
                pair = pltpu.roll(pair, 8 * q, 1)
            packed = jnp.where(owner == q, pair, packed)
        col_pack[...] = packed

    tall_size = nr * halves
    totals = [None] * PARTS
    ids = lax.broadcasted_iota(jnp.int32, (max(tall_size, WIDE), LANES), 0).astype(jnp.float32).astype(jnp.bfloat16)
    for op in slot_loads:
        op.wait()
    live = count[0]
    wide_weight = jnp.concatenate(
        [jnp.broadcast_to(weight[k : k + 1], (16, weight.shape[1])) for k in range(weight.shape[0])], axis=1
    )
    nt = (((1,), (1,)), ((), ()))
    for i in range(chunks):
        if i == min(SEND_AT, chunks - 1):
            pack_edges()
            gathered(barrier, 1, True)
            begin(halo_sends)
            for op in plane_sends:
                op.start()
            spread(ready.at[0], 1, False)
        chunk_loads[i].wait()
        position = i * slots + lax.broadcasted_iota(jnp.int32, (1, slots), 1)
        cell = cells[i]
        column = rem_by(cell, nc)
        tall = div_by(column, WIDE) * nr + div_by(cell, nc)
        tall = tall.astype(jnp.float32).astype(jnp.bfloat16)
        short = rem_by(column, WIDE).astype(jnp.float32).astype(jnp.bfloat16)
        zero, one = jnp.zeros((), jnp.bfloat16), jnp.ones((), jnp.bfloat16)
        for k in range(PARTS):
            block = slice(k * (slots // PARTS), (k + 1) * (slots // PARTS))
            amounts = lax.dot_general(wide_weight, pbuf[i, block], nt, preferred_element_type=jnp.float32)[0:1]
            amounts = jnp.where(position[:, block] < live, amounts, 0.0).astype(jnp.bfloat16)
            left, right = [], []
            for g in range(slots // PARTS // LANES):
                part = slice(g * LANES, (g + 1) * LANES)
                spot = slice(block.start + part.start, block.start + part.stop)
                left.append(jnp.where(ids[:tall_size] == tall[:, spot], jnp.broadcast_to(amounts[:, part], (tall_size, LANES)), zero))
                right.append(jnp.where(ids[:WIDE] == short[:, spot], one, zero))
            product = lax.dot_general(
                jnp.concatenate(left, axis=1), jnp.concatenate(right, axis=1).astype(jnp.float8_e4m3fn), nt,
                preferred_element_type=jnp.float32,
            )
            totals[k] = product if totals[k] is None else totals[k] + product
    for k in range(PARTS):
        acc_parts[(layer + k) % PARTS] = totals[k].reshape(acc.shape)
    acc[...] = functools.reduce(jnp.add, [acc_parts[k] for k in range(PARTS)])

    strips[0] = jnp.transpose(acc[0, :, pl.ds(0, LANES)])[0:SUB]
    strips[1] = jnp.transpose(acc[halves - 1, :, pl.ds(WIDE - LANES, LANES)])[LANES - SUB :]
    corner_tiles = ((0, pl.ds(0, LANES)), (halves - 1, pl.ds(WIDE - LANES, LANES)))
    cur_sends, cur_arrivals = exchange(
        1,
        lambda d: acc.at[:, pl.ds((nr - SUB) * d, SUB)],
        lambda d, part: strips.at[d],
        lambda r, d: acc.at[corner_tiles[d][0], pl.ds((nr - SUB) * r, SUB), corner_tiles[d][1]],
        cur_row, cur_col, cur_corner,
    )
    n = len(plane_sends)
    cur_op = to_partner(
        acc.at[:, pl.ds((1 - layer) * (half - SUB), ext)], cur_recv, part_send.at[n], part_recv.at[n]
    )
    begin(cur_sends)
    cur_op.start()

    gathered(ready.at[0], 1, False)
    if len(reaches) > 1:
        spread(ready.at[1], reaches[1], False)

    for op in own_loads:
        op.wait()
    for l in range(nl):
        for t in range(flat):
            away_start[l, t, pl.ds(half, SUB)] = jnp.zeros((SUB, LANES), jnp.float32)
    for op in plane_sends:
        op.wait()
    receive(0, halo_arrivals, TINY)
    inward = (sub < SUB // 2) == first

    def close(q, value):
        value = jnp.where(inward, inner[q], value)
        for t, at in enumerate(lanes_of):
            raw[q, t, pl.ds(half, SUB)] = value[:, t * LANES : (t + 1) * LANES]

    for k in range(nlayer):
        for l in range(nl):
            got = row_recv[k, l]
            for q, value in ((k * nl + l, got), (nz + k * nl + l, pltpu.roll(got, SUB // 2, 0))):
                close(q, value)
    got = row_recv[0, nl]
    for q, value in ((2 * nz, got), (2 * nz + 1, pltpu.roll(got, SUB // 2, 0))):
        close(q, value)
    lane_half = lane[:half]
    lane_sub = lane[:SUB]
    inward_tile = inward[:, :LANES]
    lane_ext = lax.broadcasted_iota(jnp.int32, (ext, LANES), 1)
    rim = jnp.logical_or(lane_ext < 4, lane_ext >= LANES - 4)
    body_at = pl.ds(pl.multiple_of(SUB * layer, SUB), half)
    inner_at = pl.ds(pl.multiple_of(half * (1 - layer), SUB), SUB)
    for k in range(nlayer):
        main = jnp.where((lane_half & 7) < 4, col_recv[RIGHT, k, body_at], col_recv[LEFT, k, body_at])
        near = jnp.where((lane_sub & 7) < 4, col_recv[RIGHT, k, inner_at], col_recv[LEFT, k, inner_at])
        far = jnp.where((lane_sub & 7) < 4, corner_recv[RIGHT, k], corner_recv[LEFT, k])
        mixed = jnp.concatenate([main, jnp.where(inward_tile, near, far)], axis=0)
        spots = [(q, k * nl + q) for q in range(nl)] + [(nl + q, nz + k * nl + q) for q in range(nl)]
        if k == 0:
            spots += [(2 * nl, 2 * nz), (2 * nl + 1, 2 * nz + 1)]
        for q, plane in spots:
            turned = pltpu.roll(mixed, LANES - 8 * q, 1) if q else mixed
            raw[plane, flat] = jnp.where(rim, turned, 1.0)

    shape = (tiles, high, SUB, LANES)
    lane_at = lax.broadcasted_iota(jnp.int32, shape, 3)
    last_lane, first_lane = lane_at == LANES - 1, lane_at == 0
    spill = lax.broadcasted_iota(jnp.int32, (SUB, LANES), 0) == SUB - 1

    def comb(ref):
        return jnp.stack([ref[pl.ds(v, SUB, stride=high), :] for v in range(high)])

    def plane_of(q):
        return jnp.stack([comb(raw.at[q, t]) for t in range(tiles)])

    def keep(ref, at, value):
        ref[at] = value.reshape(tiles, ext, LANES)

    def held(ref, at):
        return ref[at].reshape(shape)

    def row_up(x):
        return jnp.concatenate([x[:, 1:], pltpu.roll(x[:, 0], SUB - 1, 1)[:, None]], axis=1)

    def row_down(x):
        return jnp.concatenate([pltpu.roll(x[:, -1], 1, 1)[:, None], x[:, :-1]], axis=1)

    def lane_up(x):
        y = pltpu.roll(x.reshape(tiles * ext, LANES), LANES - 1, 1).reshape(shape)
        return jnp.where(last_lane, jnp.concatenate([y[1:], y[:1]], axis=0), y)

    def lane_down(x):
        y = pltpu.roll(x.reshape(tiles * ext, LANES), 1, 1).reshape(shape)
        return jnp.where(first_lane, jnp.concatenate([y[-1:], y[:-1]], axis=0), y)

    def pull(z, value, upper, lower):
        rows, cols = held(rows_link, z), held(cols_link, z)
        out = rows * row_up(value) + row_down(rows * value) + cols * lane_up(value) + lane_down(cols * value)
        if upper is not None:
            out = out + held(up_link, z) * upper
        if lower is not None:
            out = out + held(up_link, z - 1) * lower
        return out

    moments = [None] * (2 * ITERS)

    def measure(j, left, right):
        both = (left * right)[:flat]
        most = jnp.sum(both[:, 1:].reshape(flat * (high - 1), SUB, LANES), axis=0)
        value = jnp.sum(both[:, 0], axis=0) + jnp.where(spill, 0.0, most)
        moments[j] = value if moments[j] is None else moments[j] + value

    for z in range(nz):
        keep(began, z, plane_of(nz + z))
    via = plane_of(2 * nz)
    resist = 0.5 / plane_of(0)
    for z in range(nz):
        keep(rows_link, z, 1.0 / (resist + row_up(resist)))
        keep(cols_link, z, 1.0 / (resist + lane_up(resist)))
        if z + 1 < nz:
            upper = 0.5 / plane_of(z + 1)
            keep(up_link, z, via / (resist + upper))
            resist = upper
    for z in range(nz):
        rows, cols = held(rows_link, z), held(cols_link, z)
        whole = rows + row_down(rows) + cols + lane_down(cols)
        if z + 1 < nz:
            whole = whole + held(up_link, z)
        if z:
            whole = whole + held(up_link, z - 1)
        if z + 1 == nz:
            whole = whole + plane_of(2 * nz + 1)
        inverse = 1.0 / whole
        keep(dinv, z, inverse)
        value = held(began, z)
        image = pull(z, value, held(began, z + 1) if z + 1 < nz else None, held(began, z - 1) if z else None)
        image = image - whole * value
        keep(grad.at[0], z, image)
        if z:
            scaled = inverse * image
            keep(field.at[0], z, scaled)
            measure(0, scaled, image)

    back = [
        to_partner(src.at[pl.ds(theirs, nl), pl.ds(0, flat)], dst, back_send.at[k], back_recv.at[k])
        for k, (src, dst) in enumerate([(grad.at[c], away.at[c]) for c in range(ITERS + 1)] + [(dinv, away_dinv)])
    ]
    back[ITERS + 1].start()

    def advance(c, z):
        source = field.at[c - 1]
        value = held(source, z)
        image = pull(z, value, held(source, z + 1) if z + 1 < nz else None, held(source, z - 1) if z else None)
        keep(grad.at[c], z, image)
        measure(2 * c - 1, value, image)
        if c < ITERS:
            scaled = held(dinv, z) * image
            keep(field.at[c], z, scaled)
            measure(2 * c, scaled, image)

    for c in range(1, ITERS + 1):
        for z in range(c + 1, nz):
            advance(c, z)

    cur_op.wait()
    receive(1, cur_arrivals, 0.0)
    whole_row = pl.ds(pl.multiple_of(own_row, SUB), half)
    inner_row = pl.ds(pl.multiple_of(own_inner, SUB), SUB)
    turned = jnp.concatenate(
        [
            cur_col[RIGHT, 0] + cur_col[RIGHT, 1],
            jnp.zeros((LANES - 2 * SUB, nr), jnp.float32),
            cur_col[LEFT, 0] + cur_col[LEFT, 1],
        ],
        axis=0,
    )
    col_turn[...] = jnp.transpose(turned)
    for t in range(tiles):
        if t < flat:
            h, at = t // (WIDE // LANES), pl.ds(t % (WIDE // LANES) * LANES, LANES)
            main = acc[h, whole_row, at] + cur_recv[h, body_at, at]
            near = acc[h, inner_row, at] + cur_recv[h, inner_at, at]
            far = cur_row[0, h, :, at] + cur_row[1, h, :, at]
        else:
            main = col_turn[whole_row]
            near = col_turn[inner_row]
            far = jnp.where(
                lane_sub < LANES // 2, cur_corner[RIGHT, 0] + cur_corner[RIGHT, 1], cur_corner[LEFT, 0] + cur_corner[LEFT, 1]
            )
        cur[t, pl.ds(0, half)] = main
        cur[t, pl.ds(half, SUB)] = jnp.where(inward_tile, near, far)
    image = held(grad.at[0], 0) + jnp.stack([comb(cur.at[t]) for t in range(tiles)])
    keep(grad.at[0], 0, image)
    scaled = held(dinv, 0) * image
    keep(field.at[0], 0, scaled)
    measure(0, scaled, image)
    back[0].start()
    for c in range(1, ITERS + 1):
        for z in range(min(c + 1, nz)):
            advance(c, z)
        back[c].start()

    row = lax.broadcasted_iota(jnp.int32, (1, LANES), 1)
    packed = jnp.zeros((1, LANES), jnp.float32)
    for j, tile in enumerate(moments):
        one_row = jnp.sum(tile, axis=0, keepdims=True)
        packed = jnp.where(row == j, jnp.sum(one_row, axis=1, keepdims=True), packed)
    sums[...] = packed
    gather[me] = packed
    for k in range(1, len(reaches)):
        gathered(ready.at[k], reaches[k], False)
        if k + 1 < len(reaches):
            spread(ready.at[k + 1], reaches[k + 1], False)
    peers(
        lambda device: pltpu.make_async_remote_copy(
            src_ref=sums, dst_ref=gather.at[me], send_sem=gsend, recv_sem=grecv,
            device_id=device, device_id_type=MESH,
        ).start()
    )
    for op in back:
        op.wait()
    sent(halo_sends)
    sent(cur_sends)
    most = gather.at[pl.ds(0, total - 1)]
    pltpu.make_async_copy(most, most, grecv).wait()
    pltpu.make_async_copy(most, most, gsend).wait()
    summed = jnp.sum(gather[...], axis=0)
    totals = [jnp.sum(jnp.where(row == j, summed, 0.0), axis=1, keepdims=True) for j in range(2 * ITERS)]
    moved, scaled = cg_coefficients(totals)
    for l in range(nl):
        for t in range(flat):
            for h, parts, inverse, start in (
                (layer, [grad[c, mine + l, t] for c in range(ITERS + 1)], dinv[mine + l, t], began[mine + l, t]),
                (1 - layer, [away[c, l, t] for c in range(ITERS + 1)], away_dinv[l, t], comb(away_start.at[l, t])),
            ):
                parts = [part.reshape(high, SUB, LANES) for part in parts]
                step = moved[0] * parts[0]
                for c in range(1, ITERS):
                    step = step + moved[c] * parts[c]
                step = start.reshape(high, SUB, LANES) + inverse.reshape(high, SUB, LANES) * step
                rest = scaled[0] * parts[0]
                for c in range(1, ITERS + 1):
                    rest = rest + scaled[c] * parts[c]
                for v in range(high):
                    drop[h, l, t, pl.ds(v, SUB, stride=high), :] = step[v]
                    residual[h, l, t, pl.ds(v, SUB, stride=high), :] = rest[v]


def put(half, drop_in, residual_in, drop, residual, sem):
    ops = []
    for src, dst in ((drop_in, drop), (residual_in, residual)):
        for h in range(src.shape[0]):
            for t in range(src.shape[2]):
                place = dst.at[:, pl.ds(h * half, half), pl.ds(t * LANES, LANES)]
                ops.append(pltpu.make_async_copy(src.at[h, :, t, pl.ds(0, half)], place, sem.at[len(ops)]))
    for op in ops:
        op.start()
    for op in ops:
        op.wait()


def per_device(sizes, profiles, time_weight, slot_cell, inst_count, metal, via_density, pad, start_drop):
    nl, nr, nc = metal.shape
    inst, times = profiles.shape[-2:]
    slots = min(1024, inst)
    chunks = inst // slots
    total = sizes[0] * sizes[1] * sizes[2]
    nlayer = sizes[2]
    nz, half = nl * nlayer, nr // nlayer
    ext, tiles, halves = half + SUB, nc // LANES + 1, nc // WIDE
    kinds, pairs, count = 2 * nl + 2, nl + 1, ITERS + 1
    vmem = pl.BlockSpec(memory_space=pltpu.VMEM)
    hbm = pl.BlockSpec(memory_space=pltpu.HBM)
    stay = functools.partial(pltpu.with_memory_space_constraint, memory_space=pltpu.HBM)
    out = jax.ShapeDtypeStruct((nl, nr, nc), jnp.float32)

    def room(*shape):
        return pltpu.VMEM(shape, jnp.float32)

    DMA = pltpu.SemaphoreType.DMA
    tiled = jax.ShapeDtypeStruct((nlayer, nl, tiles - 1, ext, LANES), jnp.float32)
    results = pl.pallas_call(
        functools.partial(kernel, sizes, slots),
        out_shape=(tiled, tiled),
        in_specs=[hbm, hbm, hbm, vmem, hbm, hbm, hbm, hbm],
        out_specs=(vmem, vmem),
        scratch_shapes=[
            pltpu.VMEM((times // LANES, LANES), jnp.bfloat16),
            pltpu.VMEM((chunks, 1, slots), jnp.int32),
            pltpu.VMEM((chunks, slots, times), jnp.bfloat16),
            DMA((chunks,)),
            DMA((22 + 5 * (tiles - 1),)),
            room(2 * nz + 2, tiles, ext, LANES),
            room(2 * nz + 2, SUB, nc),
            room(2, kinds, SUB, nc),
            room(2, kinds, nr, LANES),
            room(2, pairs, SUB, nc),
            room(nr, LANES),
            room(nlayer, pairs, SUB, nc),
            room(2, nlayer, ext, LANES),
            room(2, nlayer, SUB, LANES),
            room(PARTS, halves, nr, WIDE),
            room(halves, nr, WIDE),
            room(2, SUB, nr),
            room(halves, ext, WIDE),
            room(nlayer, halves, SUB, WIDE),
            room(2, nlayer, SUB, nr),
            room(2, nlayer, SUB, LANES),
            room(nr, LANES),
            room(tiles, ext, LANES),
            room(nz, tiles, ext, LANES),
            room(nz, tiles, ext, LANES),
            room(nz, tiles, ext, LANES),
            room(nz - 1, tiles, ext, LANES),
            room(nz, tiles, ext, LANES),
            room(ITERS, nz, tiles, ext, LANES),
            room(count, nz, tiles, ext, LANES),
            room(count, nl, tiles - 1, ext, LANES),
            room(nl, tiles - 1, ext, LANES),
            room(nl, tiles - 1, ext, LANES),
            room(1, LANES),
            room(total, 1, LANES),
            DMA((2, 10)),
            DMA((2, 10)),
            DMA((2 * tiles + 1,)),
            DMA((2 * tiles + 1,)),
            DMA((count + 1,)),
            DMA((count + 1,)),
            DMA,
            DMA,
            pltpu.SemaphoreType.REGULAR((max(sizes[:2]).bit_length(),)),
        ],
        compiler_params=pltpu.CompilerParams(
            collective_id=0, has_side_effects=True, vmem_limit_bytes=48 * 1024 * 1024
        ),
    )(
        stay(profiles.reshape(chunks, slots, times)), stay(time_weight.reshape(times // LANES, LANES)),
        stay(slot_cell.reshape(chunks, 1, slots)), inst_count,
        stay(metal), stay(via_density), stay(pad), stay(start_drop),
    )
    return pl.pallas_call(
        functools.partial(put, half),
        out_shape=(out, out),
        in_specs=[vmem, vmem],
        out_specs=(hbm, hbm),
        scratch_shapes=[DMA((4 * (tiles - 1),))],
    )(*[pltpu.with_memory_space_constraint(result, memory_space=pltpu.VMEM) for result in results])


def solution(mesh):
    sizes = tuple(mesh.shape[axis] for axis in ("gx", "gy", "layer"))
    in_specs = (
        P("layer", "gx", "gy", None),
        P(),
        P("layer", "gx", "gy"),
        P("layer", "gx", "gy"),
        P("layer", "gx", "gy"),
        P("gx", "gy"),
        P("gx", "gy"),
        P("layer", "gx", "gy"),
    )
    out_specs = (P("layer", "gx", "gy"), P("layer", "gx", "gy"))
    return jax.shard_map(
        functools.partial(per_device, sizes), mesh=mesh, in_specs=in_specs, out_specs=out_specs, check_vma=False
    )
```

```python
import functools

import jax
import jax.numpy as jnp
from jax import lax
from jax.experimental import pallas as pl
from jax.experimental.pallas import tpu as pltpu
from jax.sharding import PartitionSpec as P

ITERS = 3
LANES = 128
SUB = 8
WIDE = 256
TINY = 5e-31
SEND_AT = 1
PARTS = 2
GROUP = 4
MESH = pl.DeviceIdType.MESH


def div_by(values, size):
    if size & (size - 1) == 0:
        return lax.shift_right_logical(values, jnp.full_like(values, size.bit_length() - 1))
    return lax.div(values, size)


def rem_by(values, size):
    return values & (size - 1) if size & (size - 1) == 0 else lax.rem(values, size)


def cg_coefficients(moments):
    def form(left, right):
        total = None
        for a, x in enumerate(left):
            for b, y in enumerate(right):
                term = x * y * moments[a + b]
                total = term if total is None else total + term
        return total

    one = jnp.ones_like(moments[0])
    scaled, direction = [one], [one]
    moved = [jnp.zeros_like(one)] * ITERS
    energy = form(scaled, scaled)
    for iteration in range(ITERS):
        image = [
            (direction[c] if c < len(direction) else 0.0) - (direction[c - 1] if c else 0.0)
            for c in range(len(direction) + 1)
        ]
        step = energy / form(direction, image)
        for c, value in enumerate(direction):
            moved[c] = moved[c] + step * value
        scaled = [
            (scaled[c] if c < len(scaled) else 0.0) - step * image[c] for c in range(len(image))
        ]
        if iteration + 1 < ITERS:
            energy_next = form(scaled, scaled)
            momentum = energy_next / energy
            direction = [
                scaled[c] + (momentum * direction[c] if c < len(direction) else 0.0)
                for c in range(len(scaled))
            ]
            energy = energy_next
    return moved, scaled


def kernel(
    sizes, slots, profiles, weight_in, cells_in, count, metal_in, via_in, pad_in, start_in, drop, residual,
    weight, cells, pbuf, psem, isem,
    raw, inner, row_src, col_src, row_pack, col_pack, row_recv, col_recv, corner_recv,
    acc_parts, acc, strips, cur_recv, cur_row, cur_col, cur_corner, col_turn, cur,
    began, resist, flat_planes, rows_link, cols_link, up_link, dinv, field, grad, moments, away, away_dinv, away_start,
    sums, gather, send_sem, recv_sem, part_send, part_recv, back_send, back_recv, gsend, grecv, ready,
):
    ngx, ngy, nlayer = sizes
    total = ngx * ngy * nlayer
    nl, nr, nc = metal_in.shape
    nz = nlayer * nl
    half = nr // nlayer
    ext = half + SUB
    high = ext // SUB
    flat = nc // LANES
    tiles = flat + 1
    halves = nc // WIDE
    gx, gy, layer = lax.axis_index("gx"), lax.axis_index("gy"), lax.axis_index("layer")
    me = (gx * ngy + gy) * nlayer + layer
    chunks = pbuf.shape[0]
    first = layer == 0
    mine = layer * nl
    theirs = (1 - layer) * nl
    own_row = layer * half
    other_row = (1 - layer) * half
    own_inner = half - SUB * layer
    other_inner = half - SUB * (1 - layer)

    def coords(number):
        return (number // (ngy * nlayer), (number // nlayer) % ngy, number % nlayer)

    loads = []

    def load(src, dst):
        op = pltpu.make_async_copy(src, dst, isem.at[len(loads)])
        loads.append(op)
        return op

    def edges(ref, at):
        cut = ref.at[:, pl.ds(0, SUB)], ref.at[:, pl.ds(nr - SUB, SUB)]
        side = ref.at[:, :, pl.ds(0, LANES)], ref.at[:, :, pl.ds(nc - LANES, LANES)]
        return [load(cut[d], row_src.at[d, pl.ds(at, nl)]) for d in (0, 1)] + [
            load(side[d], col_src.at[d, pl.ds(at, nl)]) for d in (0, 1)
        ]

    def flat_edges(ref, at):
        cut = ref.at[pl.ds(0, SUB)], ref.at[pl.ds(nr - SUB, SUB)]
        side = ref.at[:, pl.ds(0, LANES)], ref.at[:, pl.ds(nc - LANES, LANES)]
        return [load(cut[d], row_src.at[d, at]) for d in (0, 1)] + [load(side[d], col_src.at[d, at]) for d in (0, 1)]

    edge_loads = edges(metal_in, 0) + edges(start_in, nl) + flat_edges(via_in, 2 * nl) + flat_edges(pad_in, 2 * nl + 1)
    slot_loads = [load(weight_in, weight), load(cells_in, cells)]
    own_loads = []
    lanes_of = [pl.ds(t * LANES, LANES) for t in range(flat)]
    for k, ref in enumerate((metal_in, start_in)):
        for t, at in enumerate(lanes_of):
            own_loads.append(load(ref.at[:, pl.ds(own_row, half), at], raw.at[pl.ds(k * nz + mine, nl), t, pl.ds(0, half)]))
        own_loads.append(load(ref.at[:, pl.ds(own_inner, SUB)], inner.at[pl.ds(k * nz + mine, nl)]))
    for k, ref in enumerate((via_in, pad_in)):
        for t, at in enumerate(lanes_of):
            own_loads.append(load(ref.at[pl.ds(own_row, half), at], raw.at[2 * nz + k, t, pl.ds(0, half)]))
        own_loads.append(load(ref.at[pl.ds(own_inner, SUB)], inner.at[2 * nz + k]))
    for t, at in enumerate(lanes_of):
        own_loads.append(load(start_in.at[:, pl.ds(other_row, half), at], away_start.at[:, t, pl.ds(0, half)]))
    chunk_loads = [pltpu.make_async_copy(profiles.at[i], pbuf.at[i], psem.at[i]) for i in range(chunks)]
    for op in slot_loads + chunk_loads[:GROUP] + edge_loads + chunk_loads[GROUP:] + own_loads:
        op.start()

    barrier = pltpu.get_barrier_semaphore()

    def other(at, offset, size):
        return at ^ offset if size & (size - 1) == 0 else lax.rem(at + offset, size)

    def peers(visit):
        if total <= 64:
            offsets = [(a, b, c) for a in range(ngx) for b in range(ngy) for c in range(nlayer)]
            for a, b, c in sorted(offsets[1:], key=lambda o: -(o[0].bit_count() + o[1] + 0.5 * o[2])):
                visit((other(gx, a, ngx), other(gy, b, ngy), other(layer, c, nlayer)))
        else:
            def one(k, carry):
                visit(coords(lax.rem(me + k, total)))
                return carry

            lax.fori_loop(1, total, one, 0)

    def within(at, step, size):
        return jnp.logical_and(at + step >= 0, at + step < size)

    def spread(semaphore, reach, both_layers):
        for a in (-reach, 0, reach):
            for b in (-reach, 0, reach):
                for c in range(nlayer if both_layers else 1):
                    if (a, b, c) == (0, 0, 0) or abs(a) >= ngx or abs(b) >= ngy:
                        continue

                    @pl.when(jnp.logical_and(within(gx, a, ngx), within(gy, b, ngy)))
                    def _():
                        device = (lax.clamp(0, gx + a, ngx - 1), lax.clamp(0, gy + b, ngy - 1), other(layer, c, nlayer))
                        pl.semaphore_signal(semaphore, inc=1, device_id=device, device_id_type=MESH)

    def gathered(semaphore, reach, both_layers):
        def count(at, size):
            return 1 + (at >= reach).astype(jnp.int32) + (at + reach < size).astype(jnp.int32)

        spots = count(gx, ngx) * count(gy, ngy)
        pl.semaphore_wait(semaphore, spots * (nlayer if both_layers else 1) - 1)

    spread(barrier, 1, True)
    reaches = [1]
    while 2 * reaches[-1] < max(ngx, ngy) - 1:
        reaches.append(2 * reaches[-1])

    above, below, before, after = gx > 0, gx < ngx - 1, gy > 0, gy < ngy - 1
    gx_up, gx_down = lax.max(gx - 1, 0), lax.min(gx + 1, ngx - 1)
    gy_left, gy_right = lax.max(gy - 1, 0), lax.min(gy + 1, ngy - 1)
    outside = jnp.logical_or(jnp.logical_and(first, above), jnp.logical_and(jnp.logical_not(first), below))
    RIGHT, LEFT = 0, 1

    def exchange(stage, row_of, col_of, corner_of, row_to, col_to, corner_to):
        both = jnp.logical_and
        plan = [
            (above, (gx_up, gy, 1), row_of(0), row_to.at[layer], layer),
            (below, (gx_down, gy, 0), row_of(1), row_to.at[layer], layer),
        ]
        for there, at, side, edge_at in ((before, gy_left, RIGHT, 0), (after, gy_right, LEFT, 1)):
            for part in range(nlayer):
                plan.append((there, (gx, at, part), col_of(edge_at, part), col_to.at[side, layer], 2 + 2 * side + layer))
            plan.append((both(above, there), (gx_up, at, 1), corner_of(0, edge_at), corner_to.at[side, layer], 6 + 2 * side + layer))
            plan.append((both(below, there), (gx_down, at, 0), corner_of(1, edge_at), corner_to.at[side, layer], 6 + 2 * side + layer))
        sends = [
            (
                there,
                pltpu.make_async_remote_copy(
                    src_ref=src, dst_ref=dst, send_sem=send_sem.at[stage, k], recv_sem=recv_sem.at[stage, r],
                    device_id=device, device_id_type=MESH,
                ),
            )
            for k, (there, device, src, dst, r) in enumerate(plan)
        ]
        arrivals = [(outside, row_to, 0)]
        for there, side in ((after, RIGHT), (before, LEFT)):
            arrivals.append((there, col_to.at[side], 2 + 2 * side))
            arrivals.append((both(outside, there), corner_to.at[side], 6 + 2 * side))
        return sends, arrivals

    def begin(sends):
        for there, op in sends:
            @pl.when(there)
            def _():
                op.start()

    def sent(sends):
        for there, op in sends:
            @pl.when(there)
            def _():
                op.wait_send()

    def receive(stage, arrivals, blank):
        for there, place, at in arrivals:
            @pl.when(there)
            def _():
                for k in range(nlayer):
                    pltpu.make_async_copy(place.at[k], place.at[k], recv_sem.at[stage, at + k]).wait()

            @pl.when(jnp.logical_not(there))
            def _():
                place[...] = jnp.full(place.shape, blank, jnp.float32)

    partner = (gx, gy, 1 - layer)

    def to_partner(src, dst, send, recv):
        return pltpu.make_async_remote_copy(
            src_ref=src, dst_ref=dst, send_sem=send, recv_sem=recv, device_id=partner, device_id_type=MESH
        )

    window = [pl.ds(k * (half - SUB), ext) for k in range(nlayer)]
    halo_sends, halo_arrivals = exchange(
        0,
        lambda d: row_pack.at[d],
        lambda d, part: col_pack.at[window[part]],
        lambda r, d: col_pack.at[pl.ds((nr - SUB) * r, SUB)],
        row_recv, col_recv, corner_recv,
    )
    plane_sends = []
    for k, ref in enumerate((metal_in, start_in)):
        at = pl.ds(k * nz + mine, nl)
        for src, dst in [
            (ref.at[:, pl.ds(other_row, half), lanes_of[t]], raw.at[at, t, pl.ds(0, half)]) for t in range(flat)
        ] + [(ref.at[:, pl.ds(other_inner, SUB)], inner.at[at])]:
            n = len(plane_sends)
            plane_sends.append(to_partner(src, dst, part_send.at[n], part_recv.at[n]))

    sub = lax.broadcasted_iota(jnp.int32, (SUB, nc), 0)
    lane = lax.broadcasted_iota(jnp.int32, (nr, LANES), 1)
    kinds = 2 * nl + 2

    def pack_edges():
        for op in edge_loads:
            op.wait()
        pairs = [(l, nl + l) for l in range(nl)] + [(2 * nl, 2 * nl + 1)]
        for k, (a, b) in enumerate(pairs):
            low = pltpu.roll(row_src[0, b], SUB // 2, 0)
            row_pack[0, k] = jnp.where(sub < SUB // 2, row_src[0, a], low)
            low = pltpu.roll(row_src[1, b], SUB // 2, 0)
            row_pack[1, k] = jnp.where(sub < SUB // 2, low, row_src[1, a])
        owner = ((lane + 4) >> 3) & (LANES // 8 - 1)
        packed = jnp.ones((nr, LANES), jnp.float32)
        for q in range(kinds):
            pair = jnp.where(lane < LANES // 2, col_src[0, q], col_src[1, q])
            if q:
                pair = pltpu.roll(pair, 8 * q, 1)
            packed = jnp.where(owner == q, pair, packed)
        col_pack[...] = packed

    tall_size = nr * halves
    ids = lax.broadcasted_iota(jnp.int32, (max(tall_size, WIDE), LANES), 0).astype(jnp.float32).astype(jnp.bfloat16)
    for op in slot_loads:
        op.wait()
    live = count[0]
    wide_weight = jnp.concatenate(
        [jnp.broadcast_to(weight[k : k + 1], (16, weight.shape[1])) for k in range(weight.shape[0])], axis=1
    )
    nt = (((1,), (1,)), ((), ()))
    group = min(GROUP, chunks)
    acc_parts[...] = jnp.zeros_like(acc_parts)

    def scatter(step, carry):
        @pl.when(step == min(SEND_AT, chunks // group - 1))
        def _():
            pack_edges()
            gathered(barrier, 1, True)
            begin(halo_sends)
            for op in plane_sends:
                op.start()
            spread(ready.at[0], 1, False)

        totals = [None] * PARTS
        zero, one = jnp.zeros((), jnp.bfloat16), jnp.ones((), jnp.bfloat16)
        for u in range(group):
            i = step * group + u
            pltpu.make_async_copy(profiles.at[i], pbuf.at[i], psem.at[i]).wait()
        for u in range(group):
            i = step * group + u
            position = i * slots + lax.broadcasted_iota(jnp.int32, (1, slots), 1)
            cell = cells[i]
            column = rem_by(cell, nc)
            tall = div_by(column, WIDE) * nr + div_by(cell, nc)
            tall = tall.astype(jnp.float32).astype(jnp.bfloat16)
            short = rem_by(column, WIDE).astype(jnp.float32).astype(jnp.bfloat16)
            for k in range(PARTS):
                size = slots // PARTS
                amounts = lax.dot_general(
                    wide_weight, pbuf[i, k * size : (k + 1) * size], nt, preferred_element_type=jnp.float32
                )[0:1]
                amounts = jnp.where(position[:, k * size : (k + 1) * size] < live, amounts, 0.0).astype(jnp.bfloat16)
                left, right = [], []
                for g in range(size // LANES):
                    part = slice(g * LANES, (g + 1) * LANES)
                    spot = slice(k * size + part.start, k * size + part.stop)
                    left.append(jnp.where(ids[:tall_size] == tall[:, spot], jnp.broadcast_to(amounts[:, part], (tall_size, LANES)), zero))
                    right.append(jnp.where(ids[:WIDE] == short[:, spot], one, zero))
                product = lax.dot_general(
                    jnp.concatenate(left, axis=1), jnp.concatenate(right, axis=1).astype(jnp.float8_e4m3fn), nt,
                    preferred_element_type=jnp.float32,
                )
                totals[k] = product if totals[k] is None else totals[k] + product
        for k in range(PARTS):
            acc_parts[k] += totals[k].reshape(acc.shape)
        return carry

    lax.fori_loop(0, chunks // group, scatter, 0)
    acc[...] = functools.reduce(jnp.add, [acc_parts[k] for k in range(PARTS)])

    strips[0] = jnp.transpose(acc[0, :, pl.ds(0, LANES)])[0:SUB]
    strips[1] = jnp.transpose(acc[halves - 1, :, pl.ds(WIDE - LANES, LANES)])[LANES - SUB :]
    corner_tiles = ((0, pl.ds(0, LANES)), (halves - 1, pl.ds(WIDE - LANES, LANES)))
    cur_sends, cur_arrivals = exchange(
        1,
        lambda d: acc.at[:, pl.ds((nr - SUB) * d, SUB)],
        lambda d, part: strips.at[d],
        lambda r, d: acc.at[corner_tiles[d][0], pl.ds((nr - SUB) * r, SUB), corner_tiles[d][1]],
        cur_row, cur_col, cur_corner,
    )
    n = len(plane_sends)
    cur_op = to_partner(
        acc.at[:, pl.ds((1 - layer) * (half - SUB), ext)], cur_recv, part_send.at[n], part_recv.at[n]
    )
    begin(cur_sends)
    cur_op.start()

    gathered(ready.at[0], 1, False)
    if len(reaches) > 1:
        spread(ready.at[1], reaches[1], False)

    for op in own_loads:
        op.wait()
    for l in range(nl):
        for t in range(flat):
            away_start[l, t, pl.ds(half, SUB)] = jnp.zeros((SUB, LANES), jnp.float32)
    for op in plane_sends:
        op.wait()
    receive(0, halo_arrivals, TINY)
    inward = (sub < SUB // 2) == first

    def close(q, value):
        value = jnp.where(inward, inner[q], value)
        for t, at in enumerate(lanes_of):
            raw[q, t, pl.ds(half, SUB)] = value[:, t * LANES : (t + 1) * LANES]

    for k in range(nlayer):
        for l in range(nl):
            got = row_recv[k, l]
            for q, value in ((k * nl + l, got), (nz + k * nl + l, pltpu.roll(got, SUB // 2, 0))):
                close(q, value)
    got = row_recv[0, nl]
    for q, value in ((2 * nz, got), (2 * nz + 1, pltpu.roll(got, SUB // 2, 0))):
        close(q, value)
    lane_half = lane[:half]
    lane_sub = lane[:SUB]
    inward_tile = inward[:, :LANES]
    lane_ext = lax.broadcasted_iota(jnp.int32, (ext, LANES), 1)
    rim = jnp.logical_or(lane_ext < 4, lane_ext >= LANES - 4)
    body_at = pl.ds(pl.multiple_of(SUB * layer, SUB), half)
    inner_at = pl.ds(pl.multiple_of(half * (1 - layer), SUB), SUB)
    for k in range(nlayer):
        main = jnp.where((lane_half & 7) < 4, col_recv[RIGHT, k, body_at], col_recv[LEFT, k, body_at])
        near = jnp.where((lane_sub & 7) < 4, col_recv[RIGHT, k, inner_at], col_recv[LEFT, k, inner_at])
        far = jnp.where((lane_sub & 7) < 4, corner_recv[RIGHT, k], corner_recv[LEFT, k])
        mixed = jnp.concatenate([main, jnp.where(inward_tile, near, far)], axis=0)
        spots = [(q, k * nl + q) for q in range(nl)] + [(nl + q, nz + k * nl + q) for q in range(nl)]
        if k == 0:
            spots += [(2 * nl, 2 * nz), (2 * nl + 1, 2 * nz + 1)]
        for q, plane in spots:
            turned = pltpu.roll(mixed, LANES - 8 * q, 1) if q else mixed
            raw[plane, flat] = jnp.where(rim, turned, 1.0)

    shape = (tiles, high, SUB, LANES)
    lane_at = lax.broadcasted_iota(jnp.int32, shape, 3)
    last_lane, first_lane = lane_at == LANES - 1, lane_at == 0
    spill = lax.broadcasted_iota(jnp.int32, (SUB, LANES), 0) == SUB - 1

    def comb(ref):
        return jnp.stack([ref[pl.ds(v, SUB, stride=high), :] for v in range(high)])

    def plane_of(q):
        return jnp.stack([comb(raw.at[q, t]) for t in range(tiles)])

    def keep(ref, at, value):
        ref[at] = value.reshape(tiles, ext, LANES)

    def held(ref, at):
        return ref[at].reshape(shape)

    def row_up(x):
        return jnp.concatenate([x[:, 1:], pltpu.roll(x[:, 0], SUB - 1, 1)[:, None]], axis=1)

    def row_down(x):
        return jnp.concatenate([pltpu.roll(x[:, -1], 1, 1)[:, None], x[:, :-1]], axis=1)

    def lane_up(x):
        y = pltpu.roll(x.reshape(tiles * ext, LANES), LANES - 1, 1).reshape(shape)
        return jnp.where(last_lane, jnp.concatenate([y[1:], y[:1]], axis=0), y)

    def lane_down(x):
        y = pltpu.roll(x.reshape(tiles * ext, LANES), 1, 1).reshape(shape)
        return jnp.where(first_lane, jnp.concatenate([y[-1:], y[:-1]], axis=0), y)

    def pull(z, source):
        rows, cols = held(rows_link, z), held(cols_link, z)
        value = held(source, z + 1)
        out = rows * row_up(value) + row_down(rows * value) + cols * lane_up(value) + lane_down(cols * value)
        return value, out + held(up_link, z + 1) * held(source, z + 2) + held(up_link, z) * held(source, z)

    def measure(j, left, right):
        both = (left * right)[:flat]
        most = jnp.sum(both[:, 1:].reshape(flat * (high - 1), SUB, LANES), axis=0)
        moments[j] += jnp.sum(both[:, 0], axis=0) + jnp.where(spill, 0.0, most)

    blank = jnp.zeros((tiles, ext, LANES), jnp.float32)
    moments[...] = jnp.zeros_like(moments)
    for at in (0, nz + 1):
        began[at] = blank
    for c in range(ITERS):
        for at in (0, nz + 1):
            field[c, at] = blank
    resist[0] = jnp.full((tiles, ext, LANES), 0.5 / TINY, jnp.float32)
    up_link[nz] = blank
    for k in range(2):
        keep(flat_planes, k, plane_of(2 * nz + k))
    for z in range(nz):
        keep(resist, z + 1, plane_of(z))
        keep(began, z + 1, plane_of(nz + z))
    for l in range(nl):
        for t in range(flat):
            away_start[l, t] = comb(away_start.at[l, t]).reshape(ext, LANES)

    def links(z, carry):
        value = 0.5 / held(resist, z + 1)
        keep(resist, z + 1, value)
        keep(rows_link, z, 1.0 / (value + row_up(value)))
        keep(cols_link, z, 1.0 / (value + lane_up(value)))
        keep(up_link, z, held(flat_planes, 0) / (held(resist, z) + value))
        return carry

    lax.fori_loop(0, nz, links, 0)

    def opening(z, carry):
        rows, cols = held(rows_link, z), held(cols_link, z)
        whole = rows + row_down(rows) + cols + lane_down(cols) + held(up_link, z) + held(up_link, z + 1)
        whole = whole + jnp.where(z == nz - 1, held(flat_planes, 1), 0.0)
        inverse = 1.0 / whole
        keep(dinv, z, inverse)
        value, image = pull(z, began)
        image = image - whole * value
        keep(grad.at[0], z, image)
        scaled = inverse * image
        keep(field.at[0], z + 1, scaled)

        @pl.when(z > 0)
        def _():
            measure(0, scaled, image)

        return carry

    lax.fori_loop(0, nz, opening, 0)

    def back(c):
        src, dst = (dinv, away_dinv) if c is None else (grad.at[c], away.at[c])
        k = ITERS + 1 if c is None else c
        return to_partner(src.at[pl.ds(theirs, nl), pl.ds(0, flat)], dst, back_send.at[k], back_recv.at[k])

    back(None).start()

    def advance(c, z):
        value, image = pull(z, field.at[c - 1])
        keep(grad.at[c], z, image)
        scaled = held(dinv, z) * image
        keep(field.at[c], z + 1, scaled)
        measure(2 * c - 1, value, image)
        measure(2 * c, scaled, image)

    def sweep(lowest, highest, finish):
        def outer(c, carry):
            def step(z, inner_carry):
                advance(c, z)
                return inner_carry

            lax.fori_loop(lowest(c), highest(c), step, 0)
            if finish:
                back(c).start()
            return carry

        lax.fori_loop(1, ITERS + 1, outer, 0)

    sweep(lambda c: c + 1, lambda c: nz, False)

    cur_op.wait()
    receive(1, cur_arrivals, 0.0)
    whole_row = pl.ds(pl.multiple_of(own_row, SUB), half)
    inner_row = pl.ds(pl.multiple_of(own_inner, SUB), SUB)
    turned = jnp.concatenate(
        [
            cur_col[RIGHT, 0] + cur_col[RIGHT, 1],
            jnp.zeros((LANES - 2 * SUB, nr), jnp.float32),
            cur_col[LEFT, 0] + cur_col[LEFT, 1],
        ],
        axis=0,
    )
    col_turn[...] = jnp.transpose(turned)
    for t in range(tiles):
        if t < flat:
            h, at = t // (WIDE // LANES), pl.ds(t % (WIDE // LANES) * LANES, LANES)
            main = acc[h, whole_row, at] + cur_recv[h, body_at, at]
            near = acc[h, inner_row, at] + cur_recv[h, inner_at, at]
            far = cur_row[0, h, :, at] + cur_row[1, h, :, at]
        else:
            main = col_turn[whole_row]
            near = col_turn[inner_row]
            far = jnp.where(
                lane_sub < LANES // 2, cur_corner[RIGHT, 0] + cur_corner[RIGHT, 1], cur_corner[LEFT, 0] + cur_corner[LEFT, 1]
            )
        cur[t, pl.ds(0, half)] = main
        cur[t, pl.ds(half, SUB)] = jnp.where(inward_tile, near, far)
    image = held(grad.at[0], 0) + jnp.stack([comb(cur.at[t]) for t in range(tiles)])
    keep(grad.at[0], 0, image)
    scaled = held(dinv, 0) * image
    keep(field.at[0], 1, scaled)
    measure(0, scaled, image)
    back(0).start()
    sweep(lambda c: 0, lambda c: c + 1, True)

    row = lax.broadcasted_iota(jnp.int32, (1, LANES), 1)
    packed = jnp.zeros((1, LANES), jnp.float32)
    for j in range(2 * ITERS):
        tile = moments[j]
        one_row = jnp.sum(tile, axis=0, keepdims=True)
        packed = jnp.where(row == j, jnp.sum(one_row, axis=1, keepdims=True), packed)
    sums[...] = packed
    gather[me] = packed
    for k in range(1, len(reaches)):
        gathered(ready.at[k], reaches[k], False)
        if k + 1 < len(reaches):
            spread(ready.at[k + 1], reaches[k + 1], False)
    peers(
        lambda device: pltpu.make_async_remote_copy(
            src_ref=sums, dst_ref=gather.at[me], send_sem=gsend, recv_sem=grecv,
            device_id=device, device_id_type=MESH,
        ).start()
    )
    for c in [*range(ITERS + 1), None]:
        back(c).wait()
    sent(halo_sends)
    sent(cur_sends)
    most = gather.at[pl.ds(0, total - 1)]
    pltpu.make_async_copy(most, most, grecv).wait()
    pltpu.make_async_copy(most, most, gsend).wait()
    summed = jnp.sum(gather[...], axis=0)
    totals = [jnp.sum(jnp.where(row == j, summed, 0.0), axis=1, keepdims=True) for j in range(2 * ITERS)]
    moved, scaled = cg_coefficients(totals)
    def close_tile(k, carry):
        l, t = k // flat, k % flat
        for h, parts, inverse, start in (
            (layer, [grad[c, mine + l, t] for c in range(ITERS + 1)], dinv[mine + l, t], began[mine + l + 1, t]),
            (1 - layer, [away[c, l, t] for c in range(ITERS + 1)], away_dinv[l, t], away_start[l, t]),
        ):
            parts = [part.reshape(high, SUB, LANES) for part in parts]
            step = moved[0] * parts[0]
            for c in range(1, ITERS):
                step = step + moved[c] * parts[c]
            step = start.reshape(high, SUB, LANES) + inverse.reshape(high, SUB, LANES) * step
            rest = scaled[0] * parts[0]
            for c in range(1, ITERS + 1):
                rest = rest + scaled[c] * parts[c]
            for v in range(high):
                drop[h, l, t, pl.ds(v, SUB, stride=high), :] = step[v]
                residual[h, l, t, pl.ds(v, SUB, stride=high), :] = rest[v]
        return carry

    lax.fori_loop(0, nl * flat, close_tile, 0)


def put(half, drop_in, residual_in, drop, residual, sem):
    ops = []
    for src, dst in ((drop_in, drop), (residual_in, residual)):
        for h in range(src.shape[0]):
            for t in range(src.shape[2]):
                place = dst.at[:, pl.ds(h * half, half), pl.ds(t * LANES, LANES)]
                ops.append(pltpu.make_async_copy(src.at[h, :, t, pl.ds(0, half)], place, sem.at[len(ops)]))
    for op in ops:
        op.start()
    for op in ops:
        op.wait()


def per_device(sizes, profiles, time_weight, slot_cell, inst_count, metal, via_density, pad, start_drop):
    nl, nr, nc = metal.shape
    inst, times = profiles.shape[-2:]
    slots = min(1024, inst)
    chunks = inst // slots
    total = sizes[0] * sizes[1] * sizes[2]
    nlayer = sizes[2]
    nz, half = nl * nlayer, nr // nlayer
    ext, tiles, halves = half + SUB, nc // LANES + 1, nc // WIDE
    kinds, pairs, count = 2 * nl + 2, nl + 1, ITERS + 1
    vmem = pl.BlockSpec(memory_space=pltpu.VMEM)
    hbm = pl.BlockSpec(memory_space=pltpu.HBM)
    stay = functools.partial(pltpu.with_memory_space_constraint, memory_space=pltpu.HBM)
    out = jax.ShapeDtypeStruct((nl, nr, nc), jnp.float32)

    def room(*shape):
        return pltpu.VMEM(shape, jnp.float32)

    DMA = pltpu.SemaphoreType.DMA
    tiled = jax.ShapeDtypeStruct((nlayer, nl, tiles - 1, ext, LANES), jnp.float32)
    results = pl.pallas_call(
        functools.partial(kernel, sizes, slots),
        out_shape=(tiled, tiled),
        in_specs=[hbm, hbm, hbm, vmem, hbm, hbm, hbm, hbm],
        out_specs=(vmem, vmem),
        scratch_shapes=[
            pltpu.VMEM((times // LANES, LANES), jnp.bfloat16),
            pltpu.VMEM((chunks, 1, slots), jnp.int32),
            pltpu.VMEM((chunks, slots, times), jnp.bfloat16),
            DMA((chunks,)),
            DMA((22 + 5 * (tiles - 1),)),
            room(2 * nz + 2, tiles, ext, LANES),
            room(2 * nz + 2, SUB, nc),
            room(2, kinds, SUB, nc),
            room(2, kinds, nr, LANES),
            room(2, pairs, SUB, nc),
            room(nr, LANES),
            room(nlayer, pairs, SUB, nc),
            room(2, nlayer, ext, LANES),
            room(2, nlayer, SUB, LANES),
            room(PARTS, halves, nr, WIDE),
            room(halves, nr, WIDE),
            room(2, SUB, nr),
            room(halves, ext, WIDE),
            room(nlayer, halves, SUB, WIDE),
            room(2, nlayer, SUB, nr),
            room(2, nlayer, SUB, LANES),
            room(nr, LANES),
            room(tiles, ext, LANES),
            room(nz + 2, tiles, ext, LANES),
            room(nz + 1, tiles, ext, LANES),
            room(2, tiles, ext, LANES),
            room(nz, tiles, ext, LANES),
            room(nz, tiles, ext, LANES),
            room(nz + 1, tiles, ext, LANES),
            room(nz, tiles, ext, LANES),
            room(count, nz + 2, tiles, ext, LANES),
            room(count, nz, tiles, ext, LANES),
            room(2 * count, SUB, LANES),
            room(count, nl, tiles - 1, ext, LANES),
            room(nl, tiles - 1, ext, LANES),
            room(nl, tiles - 1, ext, LANES),
            room(1, LANES),
            room(total, 1, LANES),
            DMA((2, 10)),
            DMA((2, 10)),
            DMA((2 * tiles + 1,)),
            DMA((2 * tiles + 1,)),
            DMA((count + 1,)),
            DMA((count + 1,)),
            DMA,
            DMA,
            pltpu.SemaphoreType.REGULAR((max(sizes[:2]).bit_length(),)),
        ],
        compiler_params=pltpu.CompilerParams(
            collective_id=0, has_side_effects=True, vmem_limit_bytes=48 * 1024 * 1024
        ),
    )(
        stay(profiles.reshape(chunks, slots, times)), stay(time_weight.reshape(times // LANES, LANES)),
        stay(slot_cell.reshape(chunks, 1, slots)), inst_count,
        stay(metal), stay(via_density), stay(pad), stay(start_drop),
    )
    return pl.pallas_call(
        functools.partial(put, half),
        out_shape=(out, out),
        in_specs=[vmem, vmem],
        out_specs=(hbm, hbm),
        scratch_shapes=[DMA((4 * (tiles - 1),))],
    )(*[pltpu.with_memory_space_constraint(result, memory_space=pltpu.VMEM) for result in results])


def solution(mesh):
    sizes = tuple(mesh.shape[axis] for axis in ("gx", "gy", "layer"))
    in_specs = (
        P("layer", "gx", "gy", None),
        P(),
        P("layer", "gx", "gy"),
        P("layer", "gx", "gy"),
        P("layer", "gx", "gy"),
        P("gx", "gy"),
        P("gx", "gy"),
        P("layer", "gx", "gy"),
    )
    out_specs = (P("layer", "gx", "gy"), P("layer", "gx", "gy"))
    return jax.shard_map(
        functools.partial(per_device, sizes), mesh=mesh, in_specs=in_specs, out_specs=out_specs, check_vma=False
    )
```

```python
import functools

import jax
import jax.numpy as jnp
from jax import lax
from jax.experimental import pallas as pl
from jax.experimental.pallas import tpu as pltpu
from jax.sharding import PartitionSpec as P

ITERS = 3
LANES = 128
SUB = 8
WIDE = 256
TINY = 5e-31
SEND_AT = 3
DEPTH = 4
PARTS = 2
MESH = pl.DeviceIdType.MESH


def div_by(values, size):
    if size & (size - 1) == 0:
        return lax.shift_right_logical(values, jnp.full_like(values, size.bit_length() - 1))
    return lax.div(values, size)


def rem_by(values, size):
    return values & (size - 1) if size & (size - 1) == 0 else lax.rem(values, size)


def cg_coefficients(moments):
    def form(left, right):
        total = None
        for a, x in enumerate(left):
            for b, y in enumerate(right):
                term = x * y * moments[a + b]
                total = term if total is None else total + term
        return total

    one = jnp.ones_like(moments[0])
    scaled, direction = [one], [one]
    moved = [jnp.zeros_like(one)] * ITERS
    energy = form(scaled, scaled)
    for iteration in range(ITERS):
        image = [
            (direction[c] if c < len(direction) else 0.0) - (direction[c - 1] if c else 0.0)
            for c in range(len(direction) + 1)
        ]
        step = energy / form(direction, image)
        for c, value in enumerate(direction):
            moved[c] = moved[c] + step * value
        scaled = [
            (scaled[c] if c < len(scaled) else 0.0) - step * image[c] for c in range(len(image))
        ]
        if iteration + 1 < ITERS:
            energy_next = form(scaled, scaled)
            momentum = energy_next / energy
            direction = [
                scaled[c] + (momentum * direction[c] if c < len(direction) else 0.0)
                for c in range(len(scaled))
            ]
            energy = energy_next
    return moved, scaled


def kernel(
    sizes, slots, profiles, weight_in, cells_in, count, metal_in, via_in, pad_in, start_in, drop, residual,
    weight, cells, pbuf, psem, isem,
    raw, inner, row_src, col_src, row_pack, col_pack, row_recv, col_recv, corner_recv,
    acc_parts, acc, strips, cur_recv, cur_row, cur_col, cur_corner, col_turn, cur,
    began, rows_link, cols_link, up_link, dinv, field, grad, away, away_dinv, away_start,
    sums, gather, send_sem, recv_sem, part_send, part_recv, back_send, back_recv, gsend, grecv, ready,
):
    ngx, ngy, nlayer = sizes
    total = ngx * ngy * nlayer
    nl, nr, nc = metal_in.shape
    nz = nlayer * nl
    half = nr // nlayer
    ext = half + SUB
    high = ext // SUB
    flat = nc // LANES
    tiles = flat + 1
    halves = nc // WIDE
    gx, gy, layer = lax.axis_index("gx"), lax.axis_index("gy"), lax.axis_index("layer")
    me = (gx * ngy + gy) * nlayer + layer
    chunks = pbuf.shape[0]
    first = layer == 0
    mine = layer * nl
    theirs = (1 - layer) * nl
    own_row = layer * half
    other_row = (1 - layer) * half
    own_inner = half - SUB * layer
    other_inner = half - SUB * (1 - layer)

    def coords(number):
        return (number // (ngy * nlayer), (number // nlayer) % ngy, number % nlayer)

    loads = []

    def load(src, dst):
        op = pltpu.make_async_copy(src, dst, isem.at[len(loads)])
        loads.append(op)
        return op

    def edges(ref, at):
        cut = ref.at[:, pl.ds(0, SUB)], ref.at[:, pl.ds(nr - SUB, SUB)]
        side = ref.at[:, :, pl.ds(0, LANES)], ref.at[:, :, pl.ds(nc - LANES, LANES)]
        return [load(cut[d], row_src.at[d, pl.ds(at, nl)]) for d in (0, 1)] + [
            load(side[d], col_src.at[d, pl.ds(at, nl)]) for d in (0, 1)
        ]

    def flat_edges(ref, at):
        cut = ref.at[pl.ds(0, SUB)], ref.at[pl.ds(nr - SUB, SUB)]
        side = ref.at[:, pl.ds(0, LANES)], ref.at[:, pl.ds(nc - LANES, LANES)]
        return [load(cut[d], row_src.at[d, at]) for d in (0, 1)] + [load(side[d], col_src.at[d, at]) for d in (0, 1)]

    edge_loads = edges(metal_in, 0) + edges(start_in, nl) + flat_edges(via_in, 2 * nl) + flat_edges(pad_in, 2 * nl + 1)
    slot_loads = [load(weight_in, weight), load(cells_in, cells)]
    own_loads = []
    lanes_of = [pl.ds(t * LANES, LANES) for t in range(flat)]
    for k, ref in enumerate((metal_in, start_in)):
        for t, at in enumerate(lanes_of):
            own_loads.append(load(ref.at[:, pl.ds(own_row, half), at], raw.at[pl.ds(k * nz + mine, nl), t, pl.ds(0, half)]))
        own_loads.append(load(ref.at[:, pl.ds(own_inner, SUB)], inner.at[pl.ds(k * nz + mine, nl)]))
    for k, ref in enumerate((via_in, pad_in)):
        for t, at in enumerate(lanes_of):
            own_loads.append(load(ref.at[pl.ds(own_row, half), at], raw.at[2 * nz + k, t, pl.ds(0, half)]))
        own_loads.append(load(ref.at[pl.ds(own_inner, SUB)], inner.at[2 * nz + k]))
    for t, at in enumerate(lanes_of):
        own_loads.append(load(start_in.at[:, pl.ds(other_row, half), at], away_start.at[:, t, pl.ds(0, half)]))
    chunk_loads = [pltpu.make_async_copy(profiles.at[i], pbuf.at[i], psem.at[i]) for i in range(chunks)]
    for op in slot_loads + chunk_loads[:DEPTH]:
        op.start()

    barrier = pltpu.get_barrier_semaphore()

    def other(at, offset, size):
        return at ^ offset if size & (size - 1) == 0 else lax.rem(at + offset, size)

    def peers(visit):
        if total <= 64:
            offsets = [(a, b, c) for a in range(ngx) for b in range(ngy) for c in range(nlayer)]
            for a, b, c in sorted(offsets[1:], key=lambda o: -(o[0].bit_count() + o[1] + 0.5 * o[2])):
                visit((other(gx, a, ngx), other(gy, b, ngy), other(layer, c, nlayer)))
        else:
            def one(k, carry):
                visit(coords(lax.rem(me + k, total)))
                return carry

            lax.fori_loop(1, total, one, 0)

    def within(at, step, size):
        return jnp.logical_and(at + step >= 0, at + step < size)

    def spread(semaphore, reach, both_layers):
        for a in (-reach, 0, reach):
            for b in (-reach, 0, reach):
                for c in range(nlayer if both_layers else 1):
                    if (a, b, c) == (0, 0, 0) or abs(a) >= ngx or abs(b) >= ngy:
                        continue

                    @pl.when(jnp.logical_and(within(gx, a, ngx), within(gy, b, ngy)))
                    def _():
                        device = (lax.clamp(0, gx + a, ngx - 1), lax.clamp(0, gy + b, ngy - 1), other(layer, c, nlayer))
                        pl.semaphore_signal(semaphore, inc=1, device_id=device, device_id_type=MESH)

    def gathered(semaphore, reach, both_layers):
        def count(at, size):
            return 1 + (at >= reach).astype(jnp.int32) + (at + reach < size).astype(jnp.int32)

        spots = count(gx, ngx) * count(gy, ngy)
        pl.semaphore_wait(semaphore, spots * (nlayer if both_layers else 1) - 1)

    spread(barrier, 1, True)
    reaches = [1]
    while 2 * reaches[-1] < max(ngx, ngy) - 1:
        reaches.append(2 * reaches[-1])

    above, below, before, after = gx > 0, gx < ngx - 1, gy > 0, gy < ngy - 1
    gx_up, gx_down = lax.max(gx - 1, 0), lax.min(gx + 1, ngx - 1)
    gy_left, gy_right = lax.max(gy - 1, 0), lax.min(gy + 1, ngy - 1)
    outside = jnp.logical_or(jnp.logical_and(first, above), jnp.logical_and(jnp.logical_not(first), below))
    RIGHT, LEFT = 0, 1

    def exchange(stage, row_of, col_of, corner_of, row_to, col_to, corner_to):
        both = jnp.logical_and
        plan = [
            (above, (gx_up, gy, 1), row_of(0), row_to.at[layer], layer),
            (below, (gx_down, gy, 0), row_of(1), row_to.at[layer], layer),
        ]
        for there, at, side, edge_at in ((before, gy_left, RIGHT, 0), (after, gy_right, LEFT, 1)):
            for part in range(nlayer):
                plan.append((there, (gx, at, part), col_of(edge_at, part), col_to.at[side, layer], 2 + 2 * side + layer))
            plan.append((both(above, there), (gx_up, at, 1), corner_of(0, edge_at), corner_to.at[side, layer], 6 + 2 * side + layer))
            plan.append((both(below, there), (gx_down, at, 0), corner_of(1, edge_at), corner_to.at[side, layer], 6 + 2 * side + layer))
        sends = [
            (
                there,
                pltpu.make_async_remote_copy(
                    src_ref=src, dst_ref=dst, send_sem=send_sem.at[stage, k], recv_sem=recv_sem.at[stage, r],
                    device_id=device, device_id_type=MESH,
                ),
            )
            for k, (there, device, src, dst, r) in enumerate(plan)
        ]
        arrivals = [(outside, row_to, 0)]
        for there, side in ((after, RIGHT), (before, LEFT)):
            arrivals.append((there, col_to.at[side], 2 + 2 * side))
            arrivals.append((both(outside, there), corner_to.at[side], 6 + 2 * side))
        return sends, arrivals

    def begin(sends):
        for there, op in sends:
            @pl.when(there)
            def _():
                op.start()

    def sent(sends):
        for there, op in sends:
            @pl.when(there)
            def _():
                op.wait_send()

    def receive(stage, arrivals, blank):
        for there, place, at in arrivals:
            @pl.when(there)
            def _():
                for k in range(nlayer):
                    pltpu.make_async_copy(place.at[k], place.at[k], recv_sem.at[stage, at + k]).wait()

            @pl.when(jnp.logical_not(there))
            def _():
                place[...] = jnp.full(place.shape, blank, jnp.float32)

    partner = (gx, gy, 1 - layer)

    def to_partner(src, dst, send, recv):
        return pltpu.make_async_remote_copy(
            src_ref=src, dst_ref=dst, send_sem=send, recv_sem=recv, device_id=partner, device_id_type=MESH
        )

    window = [pl.ds(k * (half - SUB), ext) for k in range(nlayer)]
    halo_sends, halo_arrivals = exchange(
        0,
        lambda d: row_pack.at[d],
        lambda d, part: col_pack.at[window[part]],
        lambda r, d: col_pack.at[pl.ds((nr - SUB) * r, SUB)],
        row_recv, col_recv, corner_recv,
    )
    plane_sends = []
    for k, ref in enumerate((metal_in, start_in)):
        at = pl.ds(k * nz + mine, nl)
        for src, dst in [
            (ref.at[:, pl.ds(other_row, half), lanes_of[t]], raw.at[at, t, pl.ds(0, half)]) for t in range(flat)
        ] + [(ref.at[:, pl.ds(other_inner, SUB)], inner.at[at])]:
            n = len(plane_sends)
            plane_sends.append(to_partner(src, dst, part_send.at[n], part_recv.at[n]))

    sub = lax.broadcasted_iota(jnp.int32, (SUB, nc), 0)
    lane = lax.broadcasted_iota(jnp.int32, (nr, LANES), 1)
    kinds = 2 * nl + 2

    def pack_edges():
        for op in edge_loads:
            op.wait()
        pairs = [(l, nl + l) for l in range(nl)] + [(2 * nl, 2 * nl + 1)]
        for k, (a, b) in enumerate(pairs):
            low = pltpu.roll(row_src[0, b], SUB // 2, 0)
            row_pack[0, k] = jnp.where(sub < SUB // 2, row_src[0, a], low)
            low = pltpu.roll(row_src[1, b], SUB // 2, 0)
            row_pack[1, k] = jnp.where(sub < SUB // 2, low, row_src[1, a])
        owner = ((lane + 4) >> 3) & (LANES // 8 - 1)
        packed = jnp.ones((nr, LANES), jnp.float32)
        for q in range(kinds):
            pair = jnp.where(lane < LANES // 2, col_src[0, q], col_src[1, q])
            if q:
                pair = pltpu.roll(pair, 8 * q, 1)
            packed = jnp.where(owner == q, pair, packed)
        col_pack[...] = packed

    tall_size = nr * halves
    totals = [None] * PARTS
    ids = lax.broadcasted_iota(jnp.int32, (max(tall_size, WIDE), LANES), 0).astype(jnp.float32).astype(jnp.bfloat16)
    for op in slot_loads:
        op.wait()
    live = count[0]
    wide_weight = jnp.concatenate(
        [jnp.broadcast_to(weight[k : k + 1], (16, weight.shape[1])) for k in range(weight.shape[0])], axis=1
    )
    nt = (((1,), (1,)), ((), ()))
    for i in range(chunks):
        if i == min(SEND_AT, chunks - 1):
            pack_edges()
            gathered(barrier, 1, True)
            begin(halo_sends)
            for op in plane_sends:
                op.start()
            spread(ready.at[0], 1, False)
        chunk_loads[i].wait()
        for op in chunk_loads[i + DEPTH : i + DEPTH + 1] + (edge_loads if i == 0 else []) + (own_loads if i == min(5, chunks - 1) else []):
            op.start()
        position = i * slots + lax.broadcasted_iota(jnp.int32, (1, slots), 1)
        cell = cells[i]
        column = rem_by(cell, nc)
        tall = div_by(column, WIDE) * nr + div_by(cell, nc)
        tall = tall.astype(jnp.float32).astype(jnp.bfloat16)
        short = rem_by(column, WIDE).astype(jnp.float32).astype(jnp.bfloat16)
        zero, one = jnp.zeros((), jnp.bfloat16), jnp.ones((), jnp.bfloat16)
        for k in range(PARTS):
            block = slice(k * (slots // PARTS), (k + 1) * (slots // PARTS))
            amounts = lax.dot_general(wide_weight, pbuf[i, block], nt, preferred_element_type=jnp.float32)[0:1]
            amounts = jnp.where(position[:, block] < live, amounts, 0.0).astype(jnp.bfloat16)
            left, right = [], []
            for g in range(slots // PARTS // LANES):
                part = slice(g * LANES, (g + 1) * LANES)
                spot = slice(block.start + part.start, block.start + part.stop)
                left.append(jnp.where(ids[:tall_size] == tall[:, spot], jnp.broadcast_to(amounts[:, part], (tall_size, LANES)), zero))
                right.append(jnp.where(ids[:WIDE] == short[:, spot], one, zero))
            product = lax.dot_general(
                jnp.concatenate(left, axis=1), jnp.concatenate(right, axis=1).astype(jnp.float8_e4m3fn), nt,
                preferred_element_type=jnp.float32,
            )
            totals[k] = product if totals[k] is None else totals[k] + product
    for k in range(PARTS):
        acc_parts[(layer + k) % PARTS] = totals[k].reshape(acc.shape)
    acc[...] = functools.reduce(jnp.add, [acc_parts[k] for k in range(PARTS)])

    strips[0] = jnp.transpose(acc[0, :, pl.ds(0, LANES)])[0:SUB]
    strips[1] = jnp.transpose(acc[halves - 1, :, pl.ds(WIDE - LANES, LANES)])[LANES - SUB :]
    corner_tiles = ((0, pl.ds(0, LANES)), (halves - 1, pl.ds(WIDE - LANES, LANES)))
    cur_sends, cur_arrivals = exchange(
        1,
        lambda d: acc.at[:, pl.ds((nr - SUB) * d, SUB)],
        lambda d, part: strips.at[d],
        lambda r, d: acc.at[corner_tiles[d][0], pl.ds((nr - SUB) * r, SUB), corner_tiles[d][1]],
        cur_row, cur_col, cur_corner,
    )
    n = len(plane_sends)
    cur_op = to_partner(
        acc.at[:, pl.ds((1 - layer) * (half - SUB), ext)], cur_recv, part_send.at[n], part_recv.at[n]
    )
    begin(cur_sends)
    cur_op.start()

    gathered(ready.at[0], 1, False)
    if len(reaches) > 1:
        spread(ready.at[1], reaches[1], False)

    for op in own_loads:
        op.wait()
    for l in range(nl):
        for t in range(flat):
            away_start[l, t, pl.ds(half, SUB)] = jnp.zeros((SUB, LANES), jnp.float32)
    for op in plane_sends:
        op.wait()
    receive(0, halo_arrivals, TINY)
    inward = (sub < SUB // 2) == first

    def close(q, value):
        value = jnp.where(inward, inner[q], value)
        for t, at in enumerate(lanes_of):
            raw[q, t, pl.ds(half, SUB)] = value[:, t * LANES : (t + 1) * LANES]

    for k in range(nlayer):
        for l in range(nl):
            got = row_recv[k, l]
            for q, value in ((k * nl + l, got), (nz + k * nl + l, pltpu.roll(got, SUB // 2, 0))):
                close(q, value)
    got = row_recv[0, nl]
    for q, value in ((2 * nz, got), (2 * nz + 1, pltpu.roll(got, SUB // 2, 0))):
        close(q, value)
    lane_half = lane[:half]
    lane_sub = lane[:SUB]
    inward_tile = inward[:, :LANES]
    lane_ext = lax.broadcasted_iota(jnp.int32, (ext, LANES), 1)
    rim = jnp.logical_or(lane_ext < 4, lane_ext >= LANES - 4)
    body_at = pl.ds(pl.multiple_of(SUB * layer, SUB), half)
    inner_at = pl.ds(pl.multiple_of(half * (1 - layer), SUB), SUB)
    for k in range(nlayer):
        main = jnp.where((lane_half & 7) < 4, col_recv[RIGHT, k, body_at], col_recv[LEFT, k, body_at])
        near = jnp.where((lane_sub & 7) < 4, col_recv[RIGHT, k, inner_at], col_recv[LEFT, k, inner_at])
        far = jnp.where((lane_sub & 7) < 4, corner_recv[RIGHT, k], corner_recv[LEFT, k])
        mixed = jnp.concatenate([main, jnp.where(inward_tile, near, far)], axis=0)
        spots = [(q, k * nl + q) for q in range(nl)] + [(nl + q, nz + k * nl + q) for q in range(nl)]
        if k == 0:
            spots += [(2 * nl, 2 * nz), (2 * nl + 1, 2 * nz + 1)]
        for q, plane in spots:
            turned = pltpu.roll(mixed, LANES - 8 * q, 1) if q else mixed
            raw[plane, flat] = jnp.where(rim, turned, 1.0)

    shape = (tiles, high, SUB, LANES)
    lane_at = lax.broadcasted_iota(jnp.int32, shape, 3)
    last_lane, first_lane = lane_at == LANES - 1, lane_at == 0
    spill = lax.broadcasted_iota(jnp.int32, (SUB, LANES), 0) == SUB - 1

    def comb(ref):
        return jnp.stack([ref[pl.ds(v, SUB, stride=high), :] for v in range(high)])

    def plane_of(q):
        return jnp.stack([comb(raw.at[q, t]) for t in range(tiles)])

    def keep(ref, at, value):
        ref[at] = value.reshape(tiles, ext, LANES)

    def held(ref, at):
        return ref[at].reshape(shape)

    def row_up(x):
        return jnp.concatenate([x[:, 1:], pltpu.roll(x[:, 0], SUB - 1, 1)[:, None]], axis=1)

    def row_down(x):
        return jnp.concatenate([pltpu.roll(x[:, -1], 1, 1)[:, None], x[:, :-1]], axis=1)

    def lane_up(x):
        y = pltpu.roll(x.reshape(tiles * ext, LANES), LANES - 1, 1).reshape(shape)
        return jnp.where(last_lane, jnp.concatenate([y[1:], y[:1]], axis=0), y)

    def lane_down(x):
        y = pltpu.roll(x.reshape(tiles * ext, LANES), 1, 1).reshape(shape)
        return jnp.where(first_lane, jnp.concatenate([y[-1:], y[:-1]], axis=0), y)

    def pull(z, value, upper, lower):
        rows, cols = held(rows_link, z), held(cols_link, z)
        out = rows * row_up(value) + row_down(rows * value) + cols * lane_up(value) + lane_down(cols * value)
        if upper is not None:
            out = out + held(up_link, z) * upper
        if lower is not None:
            out = out + held(up_link, z - 1) * lower
        return out

    moments = [None] * (2 * ITERS)

    def measure(j, left, right):
        both = (left * right)[:flat]
        most = jnp.sum(both[:, 1:].reshape(flat * (high - 1), SUB, LANES), axis=0)
        value = jnp.sum(both[:, 0], axis=0) + jnp.where(spill, 0.0, most)
        moments[j] = value if moments[j] is None else moments[j] + value

    for z in range(nz):
        keep(began, z, plane_of(nz + z))
    via = plane_of(2 * nz)
    resist = 0.5 / plane_of(0)
    for z in range(nz):
        keep(rows_link, z, 1.0 / (resist + row_up(resist)))
        keep(cols_link, z, 1.0 / (resist + lane_up(resist)))
        if z + 1 < nz:
            upper = 0.5 / plane_of(z + 1)
            keep(up_link, z, via / (resist + upper))
            resist = upper
    for z in range(nz):
        rows, cols = held(rows_link, z), held(cols_link, z)
        whole = rows + row_down(rows) + cols + lane_down(cols)
        if z + 1 < nz:
            whole = whole + held(up_link, z)
        if z:
            whole = whole + held(up_link, z - 1)
        if z + 1 == nz:
            whole = whole + plane_of(2 * nz + 1)
        inverse = 1.0 / whole
        keep(dinv, z, inverse)
        value = held(began, z)
        image = pull(z, value, held(began, z + 1) if z + 1 < nz else None, held(began, z - 1) if z else None)
        image = image - whole * value
        keep(grad.at[0], z, image)
        if z:
            scaled = inverse * image
            keep(field.at[0], z, scaled)
            measure(0, scaled, image)

    back = [
        to_partner(src.at[pl.ds(theirs, nl), pl.ds(0, flat)], dst, back_send.at[k], back_recv.at[k])
        for k, (src, dst) in enumerate([(grad.at[c], away.at[c]) for c in range(ITERS + 1)] + [(dinv, away_dinv)])
    ]
    back[ITERS + 1].start()

    def advance(c, z):
        source = field.at[c - 1]
        value = held(source, z)
        image = pull(z, value, held(source, z + 1) if z + 1 < nz else None, held(source, z - 1) if z else None)
        keep(grad.at[c], z, image)
        measure(2 * c - 1, value, image)
        if c < ITERS:
            scaled = held(dinv, z) * image
            keep(field.at[c], z, scaled)
            measure(2 * c, scaled, image)

    for c in range(1, ITERS + 1):
        for z in range(c + 1, nz):
            advance(c, z)

    cur_op.wait()
    receive(1, cur_arrivals, 0.0)
    whole_row = pl.ds(pl.multiple_of(own_row, SUB), half)
    inner_row = pl.ds(pl.multiple_of(own_inner, SUB), SUB)
    turned = jnp.concatenate(
        [
            cur_col[RIGHT, 0] + cur_col[RIGHT, 1],
            jnp.zeros((LANES - 2 * SUB, nr), jnp.float32),
            cur_col[LEFT, 0] + cur_col[LEFT, 1],
        ],
        axis=0,
    )
    col_turn[...] = jnp.transpose(turned)
    for t in range(tiles):
        if t < flat:
            h, at = t // (WIDE // LANES), pl.ds(t % (WIDE // LANES) * LANES, LANES)
            main = acc[h, whole_row, at] + cur_recv[h, body_at, at]
            near = acc[h, inner_row, at] + cur_recv[h, inner_at, at]
            far = cur_row[0, h, :, at] + cur_row[1, h, :, at]
        else:
            main = col_turn[whole_row]
            near = col_turn[inner_row]
            far = jnp.where(
                lane_sub < LANES // 2, cur_corner[RIGHT, 0] + cur_corner[RIGHT, 1], cur_corner[LEFT, 0] + cur_corner[LEFT, 1]
            )
        cur[t, pl.ds(0, half)] = main
        cur[t, pl.ds(half, SUB)] = jnp.where(inward_tile, near, far)
    image = held(grad.at[0], 0) + jnp.stack([comb(cur.at[t]) for t in range(tiles)])
    keep(grad.at[0], 0, image)
    scaled = held(dinv, 0) * image
    keep(field.at[0], 0, scaled)
    measure(0, scaled, image)
    back[0].start()
    for c in range(1, ITERS + 1):
        for z in range(min(c + 1, nz)):
            advance(c, z)
        back[c].start()

    row = lax.broadcasted_iota(jnp.int32, (1, LANES), 1)
    packed = jnp.zeros((1, LANES), jnp.float32)
    for j, tile in enumerate(moments):
        one_row = jnp.sum(tile, axis=0, keepdims=True)
        packed = jnp.where(row == j, jnp.sum(one_row, axis=1, keepdims=True), packed)
    sums[...] = packed
    gather[me] = packed
    for k in range(1, len(reaches)):
        gathered(ready.at[k], reaches[k], False)
        if k + 1 < len(reaches):
            spread(ready.at[k + 1], reaches[k + 1], False)
    peers(
        lambda device: pltpu.make_async_remote_copy(
            src_ref=sums, dst_ref=gather.at[me], send_sem=gsend, recv_sem=grecv,
            device_id=device, device_id_type=MESH,
        ).start()
    )
    for op in back:
        op.wait()
    sent(halo_sends)
    sent(cur_sends)
    most = gather.at[pl.ds(0, total - 1)]
    pltpu.make_async_copy(most, most, grecv).wait()
    pltpu.make_async_copy(most, most, gsend).wait()
    summed = jnp.sum(gather[...], axis=0)
    totals = [jnp.sum(jnp.where(row == j, summed, 0.0), axis=1, keepdims=True) for j in range(2 * ITERS)]
    moved, scaled = cg_coefficients(totals)
    for l in range(nl):
        for t in range(flat):
            for h, parts, inverse, start in (
                (layer, [grad[c, mine + l, t] for c in range(ITERS + 1)], dinv[mine + l, t], began[mine + l, t]),
                (1 - layer, [away[c, l, t] for c in range(ITERS + 1)], away_dinv[l, t], comb(away_start.at[l, t])),
            ):
                parts = [part.reshape(high, SUB, LANES) for part in parts]
                step = moved[0] * parts[0]
                for c in range(1, ITERS):
                    step = step + moved[c] * parts[c]
                step = start.reshape(high, SUB, LANES) + inverse.reshape(high, SUB, LANES) * step
                rest = scaled[0] * parts[0]
                for c in range(1, ITERS + 1):
                    rest = rest + scaled[c] * parts[c]
                for v in range(high):
                    drop[h, l, t, pl.ds(v, SUB, stride=high), :] = step[v]
                    residual[h, l, t, pl.ds(v, SUB, stride=high), :] = rest[v]


def put(half, drop_in, residual_in, drop, residual, sem):
    ops = []
    for src, dst in ((drop_in, drop), (residual_in, residual)):
        for h in range(src.shape[0]):
            for t in range(src.shape[2]):
                place = dst.at[:, pl.ds(h * half, half), pl.ds(t * LANES, LANES)]
                ops.append(pltpu.make_async_copy(src.at[h, :, t, pl.ds(0, half)], place, sem.at[len(ops)]))
    for op in ops:
        op.start()
    for op in ops:
        op.wait()


def per_device(sizes, profiles, time_weight, slot_cell, inst_count, metal, via_density, pad, start_drop):
    nl, nr, nc = metal.shape
    inst, times = profiles.shape[-2:]
    slots = min(1024, inst)
    chunks = inst // slots
    total = sizes[0] * sizes[1] * sizes[2]
    nlayer = sizes[2]
    nz, half = nl * nlayer, nr // nlayer
    ext, tiles, halves = half + SUB, nc // LANES + 1, nc // WIDE
    kinds, pairs, count = 2 * nl + 2, nl + 1, ITERS + 1
    vmem = pl.BlockSpec(memory_space=pltpu.VMEM)
    hbm = pl.BlockSpec(memory_space=pltpu.HBM)
    stay = functools.partial(pltpu.with_memory_space_constraint, memory_space=pltpu.HBM)
    out = jax.ShapeDtypeStruct((nl, nr, nc), jnp.float32)

    def room(*shape):
        return pltpu.VMEM(shape, jnp.float32)

    DMA = pltpu.SemaphoreType.DMA
    tiled = jax.ShapeDtypeStruct((nlayer, nl, tiles - 1, ext, LANES), jnp.float32)
    results = pl.pallas_call(
        functools.partial(kernel, sizes, slots),
        out_shape=(tiled, tiled),
        in_specs=[hbm, hbm, hbm, vmem, hbm, hbm, hbm, hbm],
        out_specs=(vmem, vmem),
        scratch_shapes=[
            pltpu.VMEM((times // LANES, LANES), jnp.bfloat16),
            pltpu.VMEM((chunks, 1, slots), jnp.int32),
            pltpu.VMEM((chunks, slots, times), jnp.bfloat16),
            DMA((chunks,)),
            DMA((22 + 5 * (tiles - 1),)),
            room(2 * nz + 2, tiles, ext, LANES),
            room(2 * nz + 2, SUB, nc),
            room(2, kinds, SUB, nc),
            room(2, kinds, nr, LANES),
            room(2, pairs, SUB, nc),
            room(nr, LANES),
            room(nlayer, pairs, SUB, nc),
            room(2, nlayer, ext, LANES),
            room(2, nlayer, SUB, LANES),
            room(PARTS, halves, nr, WIDE),
            room(halves, nr, WIDE),
            room(2, SUB, nr),
            room(halves, ext, WIDE),
            room(nlayer, halves, SUB, WIDE),
            room(2, nlayer, SUB, nr),
            room(2, nlayer, SUB, LANES),
            room(nr, LANES),
            room(tiles, ext, LANES),
            room(nz, tiles, ext, LANES),
            room(nz, tiles, ext, LANES),
            room(nz, tiles, ext, LANES),
            room(nz - 1, tiles, ext, LANES),
            room(nz, tiles, ext, LANES),
            room(ITERS, nz, tiles, ext, LANES),
            room(count, nz, tiles, ext, LANES),
            room(count, nl, tiles - 1, ext, LANES),
            room(nl, tiles - 1, ext, LANES),
            room(nl, tiles - 1, ext, LANES),
            room(1, LANES),
            room(total, 1, LANES),
            DMA((2, 10)),
            DMA((2, 10)),
            DMA((2 * tiles + 1,)),
            DMA((2 * tiles + 1,)),
            DMA((count + 1,)),
            DMA((count + 1,)),
            DMA,
            DMA,
            pltpu.SemaphoreType.REGULAR((max(sizes[:2]).bit_length(),)),
        ],
        compiler_params=pltpu.CompilerParams(
            collective_id=0, has_side_effects=True, vmem_limit_bytes=48 * 1024 * 1024
        ),
    )(
        stay(profiles.reshape(chunks, slots, times)), stay(time_weight.reshape(times // LANES, LANES)),
        stay(slot_cell.reshape(chunks, 1, slots)), inst_count,
        stay(metal), stay(via_density), stay(pad), stay(start_drop),
    )
    return pl.pallas_call(
        functools.partial(put, half),
        out_shape=(out, out),
        in_specs=[vmem, vmem],
        out_specs=(hbm, hbm),
        scratch_shapes=[DMA((4 * (tiles - 1),))],
    )(*[pltpu.with_memory_space_constraint(result, memory_space=pltpu.VMEM) for result in results])


def solution(mesh):
    sizes = tuple(mesh.shape[axis] for axis in ("gx", "gy", "layer"))
    in_specs = (
        P("layer", "gx", "gy", None),
        P(),
        P("layer", "gx", "gy"),
        P("layer", "gx", "gy"),
        P("layer", "gx", "gy"),
        P("gx", "gy"),
        P("gx", "gy"),
        P("layer", "gx", "gy"),
    )
    out_specs = (P("layer", "gx", "gy"), P("layer", "gx", "gy"))
    return jax.shard_map(
        functools.partial(per_device, sizes), mesh=mesh, in_specs=in_specs, out_specs=out_specs, check_vma=False
    )
```

```python
import functools

import jax
import jax.numpy as jnp
from jax import lax
from jax.experimental import pallas as pl
from jax.experimental.pallas import tpu as pltpu
from jax.sharding import PartitionSpec as P

ITERS = 3
LANES = 128
SUB = 8
WIDE = 256
TINY = 5e-31
SEND_AT = 4
DEPTH = 4
PARTS = 2
MESH = pl.DeviceIdType.MESH


def div_by(values, size):
    if size & (size - 1) == 0:
        return lax.shift_right_logical(values, jnp.full_like(values, size.bit_length() - 1))
    return lax.div(values, size)


def rem_by(values, size):
    return values & (size - 1) if size & (size - 1) == 0 else lax.rem(values, size)


def cg_coefficients(moments):
    def form(left, right):
        total = None
        for a, x in enumerate(left):
            for b, y in enumerate(right):
                term = x * y * moments[a + b]
                total = term if total is None else total + term
        return total

    one = jnp.ones_like(moments[0])
    scaled, direction = [one], [one]
    moved = [jnp.zeros_like(one)] * ITERS
    energy = form(scaled, scaled)
    for iteration in range(ITERS):
        image = [
            (direction[c] if c < len(direction) else 0.0) - (direction[c - 1] if c else 0.0)
            for c in range(len(direction) + 1)
        ]
        step = energy / form(direction, image)
        for c, value in enumerate(direction):
            moved[c] = moved[c] + step * value
        scaled = [
            (scaled[c] if c < len(scaled) else 0.0) - step * image[c] for c in range(len(image))
        ]
        if iteration + 1 < ITERS:
            energy_next = form(scaled, scaled)
            momentum = energy_next / energy
            direction = [
                scaled[c] + (momentum * direction[c] if c < len(direction) else 0.0)
                for c in range(len(scaled))
            ]
            energy = energy_next
    return moved, scaled


def kernel(
    sizes, slots, profiles, weight_in, cells_in, count, metal_in, via_in, pad_in, start_in, drop, residual,
    weight, cells, pbuf, psem, isem,
    raw, inner, row_src, col_src, row_pack, col_pack, row_recv, col_recv, corner_recv,
    acc_parts, acc, strips, cur_recv, cur_row, cur_col, cur_corner, col_turn, cur,
    began, rows_link, cols_link, up_link, dinv, field, grad, away, away_dinv, away_start,
    sums, gather, send_sem, recv_sem, part_send, part_recv, back_send, back_recv, gsend, grecv, ready,
):
    ngx, ngy, nlayer = sizes
    total = ngx * ngy * nlayer
    nl, nr, nc = metal_in.shape
    nz = nlayer * nl
    half = nr // nlayer
    ext = half + SUB
    high = ext // SUB
    flat = nc // LANES
    tiles = flat + 1
    halves = nc // WIDE
    gx, gy, layer = lax.axis_index("gx"), lax.axis_index("gy"), lax.axis_index("layer")
    me = (gx * ngy + gy) * nlayer + layer
    chunks = pbuf.shape[0]
    first = layer == 0
    mine = layer * nl
    theirs = (1 - layer) * nl
    own_row = layer * half
    other_row = (1 - layer) * half
    own_inner = half - SUB * layer
    other_inner = half - SUB * (1 - layer)

    def coords(number):
        return (number // (ngy * nlayer), (number // nlayer) % ngy, number % nlayer)

    loads = []

    def load(src, dst):
        op = pltpu.make_async_copy(src, dst, isem.at[len(loads)])
        loads.append(op)
        return op

    def edges(ref, at):
        cut = ref.at[:, pl.ds(0, SUB)], ref.at[:, pl.ds(nr - SUB, SUB)]
        side = ref.at[:, :, pl.ds(0, LANES)], ref.at[:, :, pl.ds(nc - LANES, LANES)]
        return [load(cut[d], row_src.at[d, pl.ds(at, nl)]) for d in (0, 1)] + [
            load(side[d], col_src.at[d, pl.ds(at, nl)]) for d in (0, 1)
        ]

    def flat_edges(ref, at):
        cut = ref.at[pl.ds(0, SUB)], ref.at[pl.ds(nr - SUB, SUB)]
        side = ref.at[:, pl.ds(0, LANES)], ref.at[:, pl.ds(nc - LANES, LANES)]
        return [load(cut[d], row_src.at[d, at]) for d in (0, 1)] + [load(side[d], col_src.at[d, at]) for d in (0, 1)]

    edge_loads = edges(metal_in, 0) + edges(start_in, nl) + flat_edges(via_in, 2 * nl) + flat_edges(pad_in, 2 * nl + 1)
    slot_loads = [load(weight_in, weight), load(cells_in, cells)]
    own_loads = []
    lanes_of = [pl.ds(t * LANES, LANES) for t in range(flat)]
    for k, ref in enumerate((metal_in, start_in)):
        for t, at in enumerate(lanes_of):
            own_loads.append(load(ref.at[:, pl.ds(own_row, half), at], raw.at[pl.ds(k * nz + mine, nl), t, pl.ds(0, half)]))
        own_loads.append(load(ref.at[:, pl.ds(own_inner, SUB)], inner.at[pl.ds(k * nz + mine, nl)]))
    for k, ref in enumerate((via_in, pad_in)):
        for t, at in enumerate(lanes_of):
            own_loads.append(load(ref.at[pl.ds(own_row, half), at], raw.at[2 * nz + k, t, pl.ds(0, half)]))
        own_loads.append(load(ref.at[pl.ds(own_inner, SUB)], inner.at[2 * nz + k]))
    for t, at in enumerate(lanes_of):
        own_loads.append(load(start_in.at[:, pl.ds(other_row, half), at], away_start.at[:, t, pl.ds(0, half)]))
    chunk_loads = [pltpu.make_async_copy(profiles.at[i], pbuf.at[i], psem.at[i]) for i in range(chunks)]
    for op in slot_loads + chunk_loads[:DEPTH]:
        op.start()

    barrier = pltpu.get_barrier_semaphore()

    def other(at, offset, size):
        return at ^ offset if size & (size - 1) == 0 else lax.rem(at + offset, size)

    def peers(visit):
        if total <= 64:
            offsets = [(a, b, c) for a in range(ngx) for b in range(ngy) for c in range(nlayer)]
            for a, b, c in sorted(offsets[1:], key=lambda o: -(o[0].bit_count() + o[1] + 0.5 * o[2])):
                visit((other(gx, a, ngx), other(gy, b, ngy), other(layer, c, nlayer)))
        else:
            def one(k, carry):
                visit(coords(lax.rem(me + k, total)))
                return carry

            lax.fori_loop(1, total, one, 0)

    def within(at, step, size):
        return jnp.logical_and(at + step >= 0, at + step < size)

    def spread(semaphore, reach, both_layers):
        for a in (-reach, 0, reach):
            for b in (-reach, 0, reach):
                for c in range(nlayer if both_layers else 1):
                    if (a, b, c) == (0, 0, 0) or abs(a) >= ngx or abs(b) >= ngy:
                        continue

                    @pl.when(jnp.logical_and(within(gx, a, ngx), within(gy, b, ngy)))
                    def _():
                        device = (lax.clamp(0, gx + a, ngx - 1), lax.clamp(0, gy + b, ngy - 1), other(layer, c, nlayer))
                        pl.semaphore_signal(semaphore, inc=1, device_id=device, device_id_type=MESH)

    def gathered(semaphore, reach, both_layers):
        def count(at, size):
            return 1 + (at >= reach).astype(jnp.int32) + (at + reach < size).astype(jnp.int32)

        spots = count(gx, ngx) * count(gy, ngy)
        pl.semaphore_wait(semaphore, spots * (nlayer if both_layers else 1) - 1)

    spread(barrier, 1, True)
    reaches = [1]
    while 2 * reaches[-1] < max(ngx, ngy) - 1:
        reaches.append(2 * reaches[-1])

    above, below, before, after = gx > 0, gx < ngx - 1, gy > 0, gy < ngy - 1
    gx_up, gx_down = lax.max(gx - 1, 0), lax.min(gx + 1, ngx - 1)
    gy_left, gy_right = lax.max(gy - 1, 0), lax.min(gy + 1, ngy - 1)
    outside = jnp.logical_or(jnp.logical_and(first, above), jnp.logical_and(jnp.logical_not(first), below))
    RIGHT, LEFT = 0, 1

    def exchange(stage, row_of, col_of, corner_of, row_to, col_to, corner_to):
        both = jnp.logical_and
        plan = [
            (above, (gx_up, gy, 1), row_of(0), row_to.at[layer], layer),
            (below, (gx_down, gy, 0), row_of(1), row_to.at[layer], layer),
        ]
        for there, at, side, edge_at in ((before, gy_left, RIGHT, 0), (after, gy_right, LEFT, 1)):
            for part in range(nlayer):
                plan.append((there, (gx, at, part), col_of(edge_at, part), col_to.at[side, layer], 2 + 2 * side + layer))
            plan.append((both(above, there), (gx_up, at, 1), corner_of(0, edge_at), corner_to.at[side, layer], 6 + 2 * side + layer))
            plan.append((both(below, there), (gx_down, at, 0), corner_of(1, edge_at), corner_to.at[side, layer], 6 + 2 * side + layer))
        sends = [
            (
                there,
                pltpu.make_async_remote_copy(
                    src_ref=src, dst_ref=dst, send_sem=send_sem.at[stage, k], recv_sem=recv_sem.at[stage, r],
                    device_id=device, device_id_type=MESH,
                ),
            )
            for k, (there, device, src, dst, r) in enumerate(plan)
        ]
        arrivals = [(outside, row_to, 0)]
        for there, side in ((after, RIGHT), (before, LEFT)):
            arrivals.append((there, col_to.at[side], 2 + 2 * side))
            arrivals.append((both(outside, there), corner_to.at[side], 6 + 2 * side))
        return sends, arrivals

    def begin(sends):
        for there, op in sends:
            @pl.when(there)
            def _():
                op.start()

    def sent(sends):
        for there, op in sends:
            @pl.when(there)
            def _():
                op.wait_send()

    def receive(stage, arrivals, blank):
        for there, place, at in arrivals:
            @pl.when(there)
            def _():
                for k in range(nlayer):
                    pltpu.make_async_copy(place.at[k], place.at[k], recv_sem.at[stage, at + k]).wait()

            @pl.when(jnp.logical_not(there))
            def _():
                place[...] = jnp.full(place.shape, blank, jnp.float32)

    partner = (gx, gy, 1 - layer)

    def to_partner(src, dst, send, recv):
        return pltpu.make_async_remote_copy(
            src_ref=src, dst_ref=dst, send_sem=send, recv_sem=recv, device_id=partner, device_id_type=MESH
        )

    window = [pl.ds(k * (half - SUB), ext) for k in range(nlayer)]
    halo_sends, halo_arrivals = exchange(
        0,
        lambda d: row_pack.at[d],
        lambda d, part: col_pack.at[window[part]],
        lambda r, d: col_pack.at[pl.ds((nr - SUB) * r, SUB)],
        row_recv, col_recv, corner_recv,
    )
    plane_sends = []
    for k, ref in enumerate((metal_in, start_in)):
        at = pl.ds(k * nz + mine, nl)
        for src, dst in [
            (ref.at[:, pl.ds(other_row, half), lanes_of[t]], raw.at[at, t, pl.ds(0, half)]) for t in range(flat)
        ] + [(ref.at[:, pl.ds(other_inner, SUB)], inner.at[at])]:
            n = len(plane_sends)
            plane_sends.append(to_partner(src, dst, part_send.at[n], part_recv.at[n]))

    sub = lax.broadcasted_iota(jnp.int32, (SUB, nc), 0)
    lane = lax.broadcasted_iota(jnp.int32, (nr, LANES), 1)
    kinds = 2 * nl + 2

    def pack_edges():
        for op in edge_loads:
            op.wait()
        pairs = [(l, nl + l) for l in range(nl)] + [(2 * nl, 2 * nl + 1)]
        for k, (a, b) in enumerate(pairs):
            low = pltpu.roll(row_src[0, b], SUB // 2, 0)
            row_pack[0, k] = jnp.where(sub < SUB // 2, row_src[0, a], low)
            low = pltpu.roll(row_src[1, b], SUB // 2, 0)
            row_pack[1, k] = jnp.where(sub < SUB // 2, low, row_src[1, a])
        owner = ((lane + 4) >> 3) & (LANES // 8 - 1)
        packed = jnp.ones((nr, LANES), jnp.float32)
        for q in range(kinds):
            pair = jnp.where(lane < LANES // 2, col_src[0, q], col_src[1, q])
            if q:
                pair = pltpu.roll(pair, 8 * q, 1)
            packed = jnp.where(owner == q, pair, packed)
        col_pack[...] = packed

    tall_size = nr * halves
    totals = [None] * PARTS
    ids = lax.broadcasted_iota(jnp.int32, (max(tall_size, WIDE), LANES), 0).astype(jnp.float32).astype(jnp.bfloat16)
    for op in slot_loads:
        op.wait()
    live = count[0]
    wide_weight = jnp.concatenate(
        [jnp.broadcast_to(weight[k : k + 1], (16, weight.shape[1])) for k in range(weight.shape[0])], axis=1
    )
    nt = (((1,), (1,)), ((), ()))
    size = slots // PARTS

    def amounts_of(i):
        position = i * slots + lax.broadcasted_iota(jnp.int32, (1, slots), 1)
        out = []
        for k in range(PARTS):
            block = slice(k * size, (k + 1) * size)
            amounts = lax.dot_general(wide_weight, pbuf[i, block], nt, preferred_element_type=jnp.float32)[0:1]
            out.append(jnp.where(position[:, block] < live, amounts, 0.0).astype(jnp.bfloat16))
        return out

    def spread_chunk(i, amounts):
        cell = cells[i]
        column = rem_by(cell, nc)
        tall = div_by(column, WIDE) * nr + div_by(cell, nc)
        tall = tall.astype(jnp.float32).astype(jnp.bfloat16)
        short = rem_by(column, WIDE).astype(jnp.float32).astype(jnp.bfloat16)
        zero, one = jnp.zeros((), jnp.bfloat16), jnp.ones((), jnp.bfloat16)
        for k in range(PARTS):
            left, right = [], []
            for g in range(size // LANES):
                part = slice(g * LANES, (g + 1) * LANES)
                spot = slice(k * size + part.start, k * size + part.stop)
                left.append(
                    jnp.where(ids[:tall_size] == tall[:, spot], jnp.broadcast_to(amounts[k][:, part], (tall_size, LANES)), zero)
                )
                right.append(jnp.where(ids[:WIDE] == short[:, spot], one, zero))
            product = lax.dot_general(
                jnp.concatenate(left, axis=1), jnp.concatenate(right, axis=1).astype(jnp.float8_e4m3fn), nt,
                preferred_element_type=jnp.float32,
            )
            totals[k] = product if totals[k] is None else totals[k] + product

    for i in range(chunks):
        if i == min(SEND_AT, chunks - 1):
            pack_edges()
            gathered(barrier, 1, True)
            begin(halo_sends)
            for op in plane_sends:
                op.start()
            spread(ready.at[0], 1, False)
        chunk_loads[i].wait()
        for op in chunk_loads[i + DEPTH : i + DEPTH + 1] + (edge_loads if i == 0 else []) + (own_loads if i == min(8, chunks - 1) else []):
            op.start()
        ready_amounts = amounts_of(i)
        if i:
            spread_chunk(i - 1, waiting_amounts)
        waiting_amounts = ready_amounts
    spread_chunk(chunks - 1, waiting_amounts)
    for k in range(PARTS):
        acc_parts[(layer + k) % PARTS] = totals[k].reshape(acc.shape)
    acc[...] = functools.reduce(jnp.add, [acc_parts[k] for k in range(PARTS)])

    strips[0] = jnp.transpose(acc[0, :, pl.ds(0, LANES)])[0:SUB]
    strips[1] = jnp.transpose(acc[halves - 1, :, pl.ds(WIDE - LANES, LANES)])[LANES - SUB :]
    corner_tiles = ((0, pl.ds(0, LANES)), (halves - 1, pl.ds(WIDE - LANES, LANES)))
    cur_sends, cur_arrivals = exchange(
        1,
        lambda d: acc.at[:, pl.ds((nr - SUB) * d, SUB)],
        lambda d, part: strips.at[d],
        lambda r, d: acc.at[corner_tiles[d][0], pl.ds((nr - SUB) * r, SUB), corner_tiles[d][1]],
        cur_row, cur_col, cur_corner,
    )
    n = len(plane_sends)
    cur_op = to_partner(
        acc.at[:, pl.ds((1 - layer) * (half - SUB), ext)], cur_recv, part_send.at[n], part_recv.at[n]
    )
    begin(cur_sends)
    cur_op.start()

    gathered(ready.at[0], 1, False)
    if len(reaches) > 1:
        spread(ready.at[1], reaches[1], False)

    for op in own_loads:
        op.wait()
    for l in range(nl):
        for t in range(flat):
            away_start[l, t, pl.ds(half, SUB)] = jnp.zeros((SUB, LANES), jnp.float32)
    for op in plane_sends:
        op.wait()
    receive(0, halo_arrivals, TINY)
    inward = (sub < SUB // 2) == first

    def close(q, value):
        value = jnp.where(inward, inner[q], value)
        for t, at in enumerate(lanes_of):
            raw[q, t, pl.ds(half, SUB)] = value[:, t * LANES : (t + 1) * LANES]

    for k in range(nlayer):
        for l in range(nl):
            got = row_recv[k, l]
            for q, value in ((k * nl + l, got), (nz + k * nl + l, pltpu.roll(got, SUB // 2, 0))):
                close(q, value)
    got = row_recv[0, nl]
    for q, value in ((2 * nz, got), (2 * nz + 1, pltpu.roll(got, SUB // 2, 0))):
        close(q, value)
    lane_half = lane[:half]
    lane_sub = lane[:SUB]
    inward_tile = inward[:, :LANES]
    lane_ext = lax.broadcasted_iota(jnp.int32, (ext, LANES), 1)
    rim = jnp.logical_or(lane_ext < 4, lane_ext >= LANES - 4)
    body_at = pl.ds(pl.multiple_of(SUB * layer, SUB), half)
    inner_at = pl.ds(pl.multiple_of(half * (1 - layer), SUB), SUB)
    for k in range(nlayer):
        main = jnp.where((lane_half & 7) < 4, col_recv[RIGHT, k, body_at], col_recv[LEFT, k, body_at])
        near = jnp.where((lane_sub & 7) < 4, col_recv[RIGHT, k, inner_at], col_recv[LEFT, k, inner_at])
        far = jnp.where((lane_sub & 7) < 4, corner_recv[RIGHT, k], corner_recv[LEFT, k])
        mixed = jnp.concatenate([main, jnp.where(inward_tile, near, far)], axis=0)
        spots = [(q, k * nl + q) for q in range(nl)] + [(nl + q, nz + k * nl + q) for q in range(nl)]
        if k == 0:
            spots += [(2 * nl, 2 * nz), (2 * nl + 1, 2 * nz + 1)]
        for q, plane in spots:
            turned = pltpu.roll(mixed, LANES - 8 * q, 1) if q else mixed
            raw[plane, flat] = jnp.where(rim, turned, 1.0)

    shape = (tiles, high, SUB, LANES)
    lane_at = lax.broadcasted_iota(jnp.int32, shape, 3)
    last_lane, first_lane = lane_at == LANES - 1, lane_at == 0
    spill = lax.broadcasted_iota(jnp.int32, (SUB, LANES), 0) == SUB - 1

    def comb(ref):
        return jnp.stack([ref[pl.ds(v, SUB, stride=high), :] for v in range(high)])

    def plane_of(q):
        return jnp.stack([comb(raw.at[q, t]) for t in range(tiles)])

    def keep(ref, at, value):
        ref[at] = value.reshape(tiles, ext, LANES)

    def held(ref, at):
        return ref[at].reshape(shape)

    def row_up(x):
        return jnp.concatenate([x[:, 1:], pltpu.roll(x[:, 0], SUB - 1, 1)[:, None]], axis=1)

    def row_down(x):
        return jnp.concatenate([pltpu.roll(x[:, -1], 1, 1)[:, None], x[:, :-1]], axis=1)

    def lane_up(x):
        y = pltpu.roll(x.reshape(tiles * ext, LANES), LANES - 1, 1).reshape(shape)
        return jnp.where(last_lane, jnp.concatenate([y[1:], y[:1]], axis=0), y)

    def lane_down(x):
        y = pltpu.roll(x.reshape(tiles * ext, LANES), 1, 1).reshape(shape)
        return jnp.where(first_lane, jnp.concatenate([y[-1:], y[:-1]], axis=0), y)

    def pull(z, value, upper, lower):
        rows, cols = held(rows_link, z), held(cols_link, z)
        out = rows * row_up(value) + row_down(rows * value) + cols * lane_up(value) + lane_down(cols * value)
        if upper is not None:
            out = out + held(up_link, z) * upper
        if lower is not None:
            out = out + held(up_link, z - 1) * lower
        return out

    moments = [None] * (2 * ITERS)

    def measure(j, left, right):
        both = (left * right)[:flat]
        most = jnp.sum(both[:, 1:].reshape(flat * (high - 1), SUB, LANES), axis=0)
        value = jnp.sum(both[:, 0], axis=0) + jnp.where(spill, 0.0, most)
        moments[j] = value if moments[j] is None else moments[j] + value

    for z in range(nz):
        keep(began, z, plane_of(nz + z))
    via = plane_of(2 * nz)
    resist = 0.5 / plane_of(0)
    for z in range(nz):
        keep(rows_link, z, 1.0 / (resist + row_up(resist)))
        keep(cols_link, z, 1.0 / (resist + lane_up(resist)))
        if z + 1 < nz:
            upper = 0.5 / plane_of(z + 1)
            keep(up_link, z, via / (resist + upper))
            resist = upper
    for z in range(nz):
        rows, cols = held(rows_link, z), held(cols_link, z)
        whole = rows + row_down(rows) + cols + lane_down(cols)
        if z + 1 < nz:
            whole = whole + held(up_link, z)
        if z:
            whole = whole + held(up_link, z - 1)
        if z + 1 == nz:
            whole = whole + plane_of(2 * nz + 1)
        inverse = 1.0 / whole
        keep(dinv, z, inverse)
        value = held(began, z)
        image = pull(z, value, held(began, z + 1) if z + 1 < nz else None, held(began, z - 1) if z else None)
        image = image - whole * value
        keep(grad.at[0], z, image)
        if z:
            scaled = inverse * image
            keep(field.at[0], z, scaled)
            measure(0, scaled, image)

    back = [
        to_partner(src.at[pl.ds(theirs, nl), pl.ds(0, flat)], dst, back_send.at[k], back_recv.at[k])
        for k, (src, dst) in enumerate([(grad.at[c], away.at[c]) for c in range(ITERS + 1)] + [(dinv, away_dinv)])
    ]
    back[ITERS + 1].start()

    def advance(c, z):
        source = field.at[c - 1]
        value = held(source, z)
        image = pull(z, value, held(source, z + 1) if z + 1 < nz else None, held(source, z - 1) if z else None)
        keep(grad.at[c], z, image)
        measure(2 * c - 1, value, image)
        if c < ITERS:
            scaled = held(dinv, z) * image
            keep(field.at[c], z, scaled)
            measure(2 * c, scaled, image)

    for c in range(1, ITERS + 1):
        for z in range(c + 1, nz):
            advance(c, z)

    cur_op.wait()
    receive(1, cur_arrivals, 0.0)
    whole_row = pl.ds(pl.multiple_of(own_row, SUB), half)
    inner_row = pl.ds(pl.multiple_of(own_inner, SUB), SUB)
    turned = jnp.concatenate(
        [
            cur_col[RIGHT, 0] + cur_col[RIGHT, 1],
            jnp.zeros((LANES - 2 * SUB, nr), jnp.float32),
            cur_col[LEFT, 0] + cur_col[LEFT, 1],
        ],
        axis=0,
    )
    col_turn[...] = jnp.transpose(turned)
    for t in range(tiles):
        if t < flat:
            h, at = t // (WIDE // LANES), pl.ds(t % (WIDE // LANES) * LANES, LANES)
            main = acc[h, whole_row, at] + cur_recv[h, body_at, at]
            near = acc[h, inner_row, at] + cur_recv[h, inner_at, at]
            far = cur_row[0, h, :, at] + cur_row[1, h, :, at]
        else:
            main = col_turn[whole_row]
            near = col_turn[inner_row]
            far = jnp.where(
                lane_sub < LANES // 2, cur_corner[RIGHT, 0] + cur_corner[RIGHT, 1], cur_corner[LEFT, 0] + cur_corner[LEFT, 1]
            )
        cur[t, pl.ds(0, half)] = main
        cur[t, pl.ds(half, SUB)] = jnp.where(inward_tile, near, far)
    image = held(grad.at[0], 0) + jnp.stack([comb(cur.at[t]) for t in range(tiles)])
    keep(grad.at[0], 0, image)
    scaled = held(dinv, 0) * image
    keep(field.at[0], 0, scaled)
    measure(0, scaled, image)
    back[0].start()
    for c in range(1, ITERS + 1):
        for z in range(min(c + 1, nz)):
            advance(c, z)
        back[c].start()

    row = lax.broadcasted_iota(jnp.int32, (1, LANES), 1)
    packed = jnp.zeros((1, LANES), jnp.float32)
    for j, tile in enumerate(moments):
        one_row = jnp.sum(tile, axis=0, keepdims=True)
        packed = jnp.where(row == j, jnp.sum(one_row, axis=1, keepdims=True), packed)
    sums[...] = packed
    gather[me] = packed
    for k in range(1, len(reaches)):
        gathered(ready.at[k], reaches[k], False)
        if k + 1 < len(reaches):
            spread(ready.at[k + 1], reaches[k + 1], False)
    peers(
        lambda device: pltpu.make_async_remote_copy(
            src_ref=sums, dst_ref=gather.at[me], send_sem=gsend, recv_sem=grecv,
            device_id=device, device_id_type=MESH,
        ).start()
    )
    for op in back:
        op.wait()
    sent(halo_sends)
    sent(cur_sends)
    most = gather.at[pl.ds(0, total - 1)]
    pltpu.make_async_copy(most, most, grecv).wait()
    pltpu.make_async_copy(most, most, gsend).wait()
    summed = jnp.sum(gather[...], axis=0)
    totals = [jnp.sum(jnp.where(row == j, summed, 0.0), axis=1, keepdims=True) for j in range(2 * ITERS)]
    moved, scaled = cg_coefficients(totals)
    for l in range(nl):
        for t in range(flat):
            for h, parts, inverse, start in (
                (layer, [grad[c, mine + l, t] for c in range(ITERS + 1)], dinv[mine + l, t], began[mine + l, t]),
                (1 - layer, [away[c, l, t] for c in range(ITERS + 1)], away_dinv[l, t], comb(away_start.at[l, t])),
            ):
                parts = [part.reshape(high, SUB, LANES) for part in parts]
                step = moved[0] * parts[0]
                for c in range(1, ITERS):
                    step = step + moved[c] * parts[c]
                step = start.reshape(high, SUB, LANES) + inverse.reshape(high, SUB, LANES) * step
                rest = scaled[0] * parts[0]
                for c in range(1, ITERS + 1):
                    rest = rest + scaled[c] * parts[c]
                for v in range(high):
                    drop[h, l, t, pl.ds(v, SUB, stride=high), :] = step[v]
                    residual[h, l, t, pl.ds(v, SUB, stride=high), :] = rest[v]


def put(half, drop_in, residual_in, drop, residual, sem):
    ops = []
    for src, dst in ((drop_in, drop), (residual_in, residual)):
        for h in range(src.shape[0]):
            for t in range(src.shape[2]):
                place = dst.at[:, pl.ds(h * half, half), pl.ds(t * LANES, LANES)]
                ops.append(pltpu.make_async_copy(src.at[h, :, t, pl.ds(0, half)], place, sem.at[len(ops)]))
    for op in ops:
        op.start()
    for op in ops:
        op.wait()


def per_device(sizes, profiles, time_weight, slot_cell, inst_count, metal, via_density, pad, start_drop):
    nl, nr, nc = metal.shape
    inst, times = profiles.shape[-2:]
    slots = min(1024, inst)
    chunks = inst // slots
    total = sizes[0] * sizes[1] * sizes[2]
    nlayer = sizes[2]
    nz, half = nl * nlayer, nr // nlayer
    ext, tiles, halves = half + SUB, nc // LANES + 1, nc // WIDE
    kinds, pairs, count = 2 * nl + 2, nl + 1, ITERS + 1
    vmem = pl.BlockSpec(memory_space=pltpu.VMEM)
    hbm = pl.BlockSpec(memory_space=pltpu.HBM)
    stay = functools.partial(pltpu.with_memory_space_constraint, memory_space=pltpu.HBM)
    out = jax.ShapeDtypeStruct((nl, nr, nc), jnp.float32)

    def room(*shape):
        return pltpu.VMEM(shape, jnp.float32)

    DMA = pltpu.SemaphoreType.DMA
    tiled = jax.ShapeDtypeStruct((nlayer, nl, tiles - 1, ext, LANES), jnp.float32)
    results = pl.pallas_call(
        functools.partial(kernel, sizes, slots),
        out_shape=(tiled, tiled),
        in_specs=[hbm, hbm, hbm, vmem, hbm, hbm, hbm, hbm],
        out_specs=(vmem, vmem),
        scratch_shapes=[
            pltpu.VMEM((times // LANES, LANES), jnp.bfloat16),
            pltpu.VMEM((chunks, 1, slots), jnp.int32),
            pltpu.VMEM((chunks, slots, times), jnp.bfloat16),
            DMA((chunks,)),
            DMA((22 + 5 * (tiles - 1),)),
            room(2 * nz + 2, tiles, ext, LANES),
            room(2 * nz + 2, SUB, nc),
            room(2, kinds, SUB, nc),
            room(2, kinds, nr, LANES),
            room(2, pairs, SUB, nc),
            room(nr, LANES),
            room(nlayer, pairs, SUB, nc),
            room(2, nlayer, ext, LANES),
            room(2, nlayer, SUB, LANES),
            room(PARTS, halves, nr, WIDE),
            room(halves, nr, WIDE),
            room(2, SUB, nr),
            room(halves, ext, WIDE),
            room(nlayer, halves, SUB, WIDE),
            room(2, nlayer, SUB, nr),
            room(2, nlayer, SUB, LANES),
            room(nr, LANES),
            room(tiles, ext, LANES),
            room(nz, tiles, ext, LANES),
            room(nz, tiles, ext, LANES),
            room(nz, tiles, ext, LANES),
            room(nz - 1, tiles, ext, LANES),
            room(nz, tiles, ext, LANES),
            room(ITERS, nz, tiles, ext, LANES),
            room(count, nz, tiles, ext, LANES),
            room(count, nl, tiles - 1, ext, LANES),
            room(nl, tiles - 1, ext, LANES),
            room(nl, tiles - 1, ext, LANES),
            room(1, LANES),
            room(total, 1, LANES),
            DMA((2, 10)),
            DMA((2, 10)),
            DMA((2 * tiles + 1,)),
            DMA((2 * tiles + 1,)),
            DMA((count + 1,)),
            DMA((count + 1,)),
            DMA,
            DMA,
            pltpu.SemaphoreType.REGULAR((max(sizes[:2]).bit_length(),)),
        ],
        compiler_params=pltpu.CompilerParams(
            collective_id=0, has_side_effects=True, vmem_limit_bytes=48 * 1024 * 1024
        ),
    )(
        stay(profiles.reshape(chunks, slots, times)), stay(time_weight.reshape(times // LANES, LANES)),
        stay(slot_cell.reshape(chunks, 1, slots)), inst_count,
        stay(metal), stay(via_density), stay(pad), stay(start_drop),
    )
    return pl.pallas_call(
        functools.partial(put, half),
        out_shape=(out, out),
        in_specs=[vmem, vmem],
        out_specs=(hbm, hbm),
        scratch_shapes=[DMA((4 * (tiles - 1),))],
    )(*[pltpu.with_memory_space_constraint(result, memory_space=pltpu.VMEM) for result in results])


def solution(mesh):
    sizes = tuple(mesh.shape[axis] for axis in ("gx", "gy", "layer"))
    in_specs = (
        P("layer", "gx", "gy", None),
        P(),
        P("layer", "gx", "gy"),
        P("layer", "gx", "gy"),
        P("layer", "gx", "gy"),
        P("gx", "gy"),
        P("gx", "gy"),
        P("layer", "gx", "gy"),
    )
    out_specs = (P("layer", "gx", "gy"), P("layer", "gx", "gy"))
    return jax.shard_map(
        functools.partial(per_device, sizes), mesh=mesh, in_specs=in_specs, out_specs=out_specs, check_vma=False
    )
```
